128 devices in a mesh: aux: 8 (over z, core), orb: 16 (over x, y).
Axes of the slice: x: 4, y: 4, z: 4, core: 2. Of those that a mesh axis runs over, the one named last changes fastest.
Arguments:
- half: bfloat16 [128, 384, 3072], P('aux', 'orb'), may hold values from -1 to 1
- metric: bfloat16 [128, 128], P('aux'), may hold values from -1 to 2
- survive: int32 [8, 16, 24], P('aux', 'orb'), may hold values 0 or 1
Outputs:
- exchange_k: float32 [3072, 3072], P('orb', 'aux')
The draws below stay inside these ranges and needn't reach their ends.
All inputs are finite; a program needn't handle non-finite values. No bound on the sum of `survive` on one device may be relied on, other than what follows from the above.
Results may differ from the reference program's by a relative error of at most 0.00098.
Values may be sent and summed in bfloat16 or wider, within the bound.
A program may use at most 128 MiB of HBM per device.

```python
import jax
import jax.numpy as jnp
from jax import lax

NOCC = 384
OCCB = 24
NAO = 3072
AOBLK = 128
NAUX = 128
N_AUX = 8


def draw_metric(key, part):
    first_key = jax.random.fold_in(key, 11)
    second_key = jax.random.fold_in(key, 12)
    spread = jax.random.normal(first_key, (NAUX, NAUX), jnp.float32) * (0.6 / NAUX ** 0.5)
    diagonal_part = jax.random.uniform(second_key, (NAUX,), jnp.float32, 0.9, 1.1)
    return (spread + jnp.diag(diagonal_part)).astype(jnp.bfloat16)


def set_ends(entries, own_key, low, largest):
    shape = entries.shape
    place = [jax.random.randint(jax.random.fold_in(own_key, axis), (), 0, shape[axis]) for axis in range(len(shape))]
    entries = entries.at[tuple(place)].set(low)
    longest = shape.index(max(shape))
    place[longest] = (place[longest] + 1) % shape[longest]
    return entries.at[tuple(place)].set(largest)


def steps_of(key, shape, cuts, low, largest):
    def one(axis_at, shards_of):
        draws = jax.random.uniform(jax.random.fold_in(jax.random.fold_in(key, 6), axis_at), (shards_of,), jnp.float32, low / len(cuts), largest / len(cuts))
        return jnp.repeat(jnp.exp(draws), shape[axis_at] // shards_of).reshape((-1,) + (1,) * (len(shape) - axis_at - 1))

    level = one(*cuts[0])
    for cut in cuts[1:]:
        level = level * one(*cut)
    return level


def bell_draw(key, shape, scale, most, shards=(), kind=jnp.bfloat16):
    factor_of = steps_of(key, shape, shards, -0.22, 0.18) if shards else 1.0
    values = jax.random.normal(key, shape, jnp.float32) * scale * factor_of
    return jnp.minimum(jnp.maximum(values, -most), most).astype(kind)


def setup_inputs(seed: int = 0) -> dict:
    key_of = jax.random.split(jax.random.key(seed), 4)
    half = bell_draw(key_of[0], (NAUX, NOCC, NAO), ((NAUX * NOCC) ** -0.25), 1.0, ((0, 8), (1, 16)))
    metric = draw_metric(jax.random.fold_in(key_of[3], 71), 0)
    survive = set_ends((jax.random.randint(key_of[2], (N_AUX, NOCC // OCCB, NAO // AOBLK), 0, 3) < 2).astype(jnp.int32), jax.random.fold_in(key_of[2], 1), 0, 1)
    return dict(half=half, metric=metric, survive=survive)


def reference(half, metric, survive):
    blocks_aux, blocks_occ, blocks_ao = survive.shape
    aux_count, occ_count, ao_count = half.shape
    gate = survive.astype(jnp.bfloat16)
    shaped = half.reshape(blocks_aux, aux_count // blocks_aux, blocks_occ, occ_count // blocks_occ, blocks_ao, ao_count // blocks_ao)
    masked = (shaped * gate[:, None, :, None, :, None]).reshape(aux_count, occ_count, ao_count)
    occ_width = occ_count // blocks_occ

    def accumulate(totals, block_index):
        occ_rows = lax.dynamic_slice_in_dim(masked, block_index * occ_width, occ_width, 1)
        fitted = jnp.dot(metric, occ_rows.reshape(aux_count, -1), preferred_element_type=jnp.float32)
        fitted = fitted.astype(jnp.bfloat16).reshape(-1, ao_count)
        update = lax.dot_general(fitted, fitted, (((0,), (0,)), ((), ())), preferred_element_type=jnp.float32)
        return totals + update, None

    exchange_k, _ = lax.scan(accumulate, jnp.zeros((ao_count, ao_count), jnp.float32), jnp.arange(blocks_occ, dtype=jnp.int32))
    return exchange_k
```

```python
import jax
import jax.numpy as jnp
from jax import lax
from jax.experimental import pallas as pl
from jax.experimental.pallas import tpu as pltpu
from jax.sharding import PartitionSpec as P

MESH = pl.DeviceIdType.MESH
F32 = jnp.float32


def gated(half, survive):
    aux_local, occ_local, ao_count = half.shape
    blocks_aux, blocks_occ, blocks_ao = survive.shape
    gate = survive.astype(jnp.bfloat16)
    shaped = half.reshape(
        blocks_aux, aux_local, blocks_occ, occ_local // blocks_occ, blocks_ao, ao_count // blocks_ao
    )
    return (shaped * gate[:, None, :, None, :, None]).reshape(aux_local, occ_local, ao_count)


def plain(half, metric, survive):
    aux_local, occ_local, ao_count = half.shape
    portion = lax.all_gather(gated(half, survive), "aux", axis=0, tiled=True)
    fit_total = jnp.dot(metric, portion.reshape(portion.shape[0], -1), preferred_element_type=F32)
    fitted = fit_total.astype(jnp.bfloat16).reshape(aux_local, occ_local, ao_count)
    group_width = ao_count // lax.axis_size("orb")
    row_start = lax.axis_index("orb") * group_width
    flat_rows = lax.all_gather(fitted, "orb", axis=1, tiled=True).reshape(-1, ao_count)
    left_rows = lax.dynamic_slice_in_dim(flat_rows, row_start, group_width, 1)
    partial_k = lax.dot_general(
        left_rows, flat_rows, (((0,), (0,)), ((), ())), preferred_element_type=F32
    )
    return lax.psum_scatter(partial_k, "aux", scatter_dimension=1, tiled=True)


WAVES = (4, 2, 3, 0, 1)


def cube_kernel(
    blocks, metric_ref, out_ref, held, via, whole, fit, turned, left, kf, kb, sb, far1, p1, v, b2, far2, p2,
    ks, fin, acc, mirror, ms, mr, zfs, zfr, zns, znr, zrs, zrr, ds, dr, f1s, f1r, p1s, p1r, f2s, f2r, p2s, p2r,
    zs, zr, xs, xr,
):
    a, o = lax.axis_index("aux"), lax.axis_index("orb")
    z, c = a // 2, a % 2
    x, y = o // 4, o % 4
    ao = blocks.shape[2]
    n_own, part = blocks.shape[1], blocks.shape[0] // 4
    cut = part // 2
    naux = whole.shape[0]
    chunk, cols, rows = ao // 4, ao // 8, ao // 32
    split = rows // 2
    f_step, s_step = 4 - 3 * c, 1 + 3 * c
    f = x * (1 - c) + y * c
    s = y * (1 - c) + x * c
    partner = a + 1 - 2 * c

    def orb_at(df, dsec):
        return ((f + df) % 4) * f_step + ((s + dsec) % 4) * s_step

    def aux_at(dz):
        return ((z + dz) % 4) * 2 + c

    mirrored = z != x
    peers = [(2 * a + h, o // 2) for h in range(2)]
    barrier = pltpu.get_barrier_semaphore()

    def greet(there_a, there_o):
        pl.semaphore_signal(barrier, inc=1, device_id={"aux": there_a, "orb": there_o}, device_id_type=MESH)

    for d in range(1, 8):
        greet((a + d) % 8, o)
    for d in (1, 3):
        greet(a, orb_at(d, 0))
        greet(a, orb_at(0, d))

    @pl.when(mirrored)
    def _():
        for to_o, to_a in peers:
            greet(to_a, to_o)

    pl.semaphore_wait(barrier, 11 + 2 * jnp.where(mirrored, 1, 0))

    def remote(src, dst, send, recv, to_a, to_o):
        return pltpu.make_async_remote_copy(
            src_ref=src, dst_ref=dst, send_sem=send, recv_sem=recv,
            device_id={"aux": to_a, "orb": to_o}, device_id_type=MESH,
        )

    started = []

    def go(copy):
        copy.start()
        started.append(copy)
        return copy

    def aux_rows(aux):
        return pl.ds(pl.multiple_of(aux * n_own, n_own), n_own)

    mine = aux_rows(a)
    span = [pl.ds(k * chunk, chunk) for k in range(4)]

    def orbitals(dz, first, count):
        return pl.ds(((z + dz) % 4) * part + first, count)

    far, near, relay = {}, {}, {}

    def issue(k):
        far[k] = [
            go(remote(blocks.at[orbitals(2, 0, cut), :, span[k]], via.at[0, :, :, span[k]],
                      zfs.at[k, 0], zfr.at[k, 0], aux_at(1), o)),
            go(remote(blocks.at[orbitals(2, cut, cut), :, span[k]], via.at[1, :, :, span[k]],
                      zfs.at[k, 1], zfr.at[k, 1], aux_at(3), o)),
        ]
        near[k] = [
            go(remote(blocks.at[orbitals(dz, 0, part), :, span[k]], held.at[:, mine, span[k]],
                      zns.at[k, n], znr.at[k, n], aux_at(dz), o))
            for n, dz in enumerate((1, 3))
        ]

    issue(0)
    issue(1)
    gather = [
        go(remote(metric_ref, whole.at[mine], ms.at[d], mr.at[d], (a + d) % 8, o)) for d in range(1, 8)
    ]
    own_block = blocks.at[orbitals(0, 0, part)]
    to_partner = {"own": go(remote(own_block, held.at[:, mine], ds.at[12], dr.at[12], partner, o))}
    whole[mine, :] = metric_ref[...]
    held[:, mine, :] = own_block[...]

    def hand_over(k, n, dz):
        there = held.at[:, aux_rows(aux_at(dz)), span[k]]
        to_partner[k, n] = go(remote(there, there, ds.at[3 * k + n], dr.at[3 * k + n], partner, o))

    def finish(k):
        for copy in relay[k]:
            copy.wait_recv()
        hand_over(k, 2, 2)
        if k == 0:
            for copy in gather:
                copy.wait_recv()
            to_partner["own"].wait_recv()
        for n in range(3):
            to_partner[k, n].wait_recv()

        @pl.loop(0, part)
        def _(i):
            at = pl.ds(pl.multiple_of(i * naux, naux), naux)
            fit[at, span[k]] = jnp.dot(
                whole[...], held[i, :, span[k]], preferred_element_type=F32
            ).astype(fit.dtype)

        @pl.loop(0, chunk // 128)
        def _(t):
            at = pl.ds(pl.multiple_of(t * 128, 128), 128)
            src = pl.ds(pl.multiple_of(k * chunk + t * 128, 128), 128)
            turned[at, :] = fit[:, src].T

        for n in range(4):
            at = pl.ds(pl.multiple_of(2 * n * rows + c * rows, rows), rows)
            left[k, n * rows : (n + 1) * rows, :] = turned[at, :]

    for k in range(4):
        for copy in far[k]:
            copy.wait_recv()
        relay[k] = [
            go(remote(via.at[0, :, :, span[k]], held.at[pl.ds(0, cut), aux_rows(aux_at(3)), span[k]],
                      zrs.at[k, 0], zrr.at[k, 0], aux_at(1), o)),
            go(remote(via.at[1, :, :, span[k]], held.at[pl.ds(cut, cut), aux_rows(aux_at(1)), span[k]],
                      zrs.at[k, 1], zrr.at[k, 1], aux_at(3), o)),
        ]
        if k + 2 < 4:
            issue(k + 2)
        for copy in near[k]:
            copy.wait_recv()
        hand_over(k, 0, 3)
        hand_over(k, 1, 1)
        if k:
            finish(k - 1)
    finish(3)

    def multiply(w):
        j = WAVES[w]

        def put(g, first, block):
            at = pl.ds(pl.multiple_of(block * cols, cols), cols)
            count = 4 if j < 4 else 2
            more = jnp.dot(
                left[g, first * rows : (first + count) * rows, :], fit[:, at], preferred_element_type=F32
            )
            for n in range(count):
                tile = more[n * rows : (n + 1) * rows]
                kf[w, 4 * g + first + n] = tile
                kb[w, 4 * g + first + n] = tile.astype(kb.dtype)

        @pl.loop(0, 4)
        def _(g):
            if j < 4:
                put(g, 0, (2 * g + j) % 8)
            else:
                for n in range(2):
                    put(g, 2 * n, 2 * ((g + 2) % 4) + (n + g // 2) % 2)

    first_far, first_in, second_far, second_in, to_owner = {}, {}, {}, {}, {}

    def ring_send(w, src, up, r):
        n = 0 if up else 1
        first_in[w, n, r] = go(remote(
            src, p1.at[w, n, r], p1s.at[w, 4 * n + r], p1r.at[w, 4 * n + r], a, orb_at(1 if up else 3, 0)
        ))

    def stage1(w):
        multiply(w)
        for r in (2, 3, 1, 0):
            up = r in (1, 2)
            first_far[w, r] = go(remote(
                kb.at[w, orb_at(2, r)], far1.at[w, r], f1s.at[w, r], f1r.at[w, r], a, orb_at(1 if up else 3, 0)
            ))
        for r in (2, 3, 1, 0):
            up = r in (0, 3)
            ring_send(w, kb.at[w, orb_at(1 if up else 3, r)], up, r)

    def stage2(w):
        for r in (2, 3, 1, 0):
            up = r in (1, 2)
            first_far[w, r].wait_recv()
            sb[w, r] = (kf[w, orb_at(1 if up else 3, r)] + far1[w, r]).astype(sb.dtype)
            ring_send(w, sb.at[w, r], up, r)

    low, high = pl.ds(0, split), pl.ds(split, split)

    def stage3(w):
        for r in (2, 3, 1, 0):
            first_in[w, 0, r].wait_recv()
            first_in[w, 1, r].wait_recv()
            total = kf[w, orb_at(0, r)] + p1[w, 0, r] + p1[w, 1, r]
            if r == 2:
                b2[w, 0] = total.astype(b2.dtype)
                second_far[w, 0] = go(remote(
                    b2.at[w, 0, low], far2.at[w, 0], f2s.at[w, 0], f2r.at[w, 0], a, orb_at(0, 1)
                ))
                second_far[w, 1] = go(remote(
                    b2.at[w, 0, high], far2.at[w, 1], f2s.at[w, 1], f2r.at[w, 1], a, orb_at(0, 3)
                ))
            else:
                v[w, r] = total

    def stage4(w):
        for n, r in ((0, 1), (1, 3)):
            second_far[w, n].wait_recv()
            summed, plain_rows = (low, high) if n == 0 else (high, low)
            b2[w, 1 + n, summed] = (v[w, r, summed] + far2[w, n]).astype(b2.dtype)
            b2[w, 1 + n, plain_rows] = v[w, r, plain_rows].astype(b2.dtype)
            second_in[w, n] = go(remote(
                b2.at[w, 1 + n], p2.at[w, n], p2s.at[w, n], p2r.at[w, n], a, orb_at(0, r)
            ))

    def owner_of(w):
        j = WAVES[w]
        if j < 4:
            return 2 * ((x + j // 2) % 4) + j % 2
        return 2 * ((x + 2) % 4) + (y // 2 + x // 2) % 2

    def stage5(w):
        for n in range(2):
            second_in[w, n].wait_recv()
        owner = owner_of(w)
        total = v[w, 0] + p2[w, 0] + p2[w, 1]
        d = (owner + 8 - a) % 8
        ks[w] = total
        to_owner[w] = remote(ks.at[w], fin.at[d], zs.at[w], zr.at[d], owner, o)

        @pl.when(owner != a)
        def _():
            to_owner[w].start()

        @pl.when(owner == a)
        def _():
            fin[0] = total

    half_cols = 2 * cols // 3

    def arrive():
        for d in range(1, 8):
            remote(ks.at[0], fin.at[d], zs.at[0], zr.at[d], a, o).wait_recv()
        same = fin[0] + fin[2] + fin[4] + fin[6]
        other = fin[1] + fin[3] + fin[5] + fin[7]
        return same, other

    def place(c_rows):
        return pl.ds(pl.multiple_of(c_rows * rows, rows), rows)

    outgoing = [
        remote(acc.at[:, pl.ds(h * (cols - half_cols), half_cols)], mirror.at[o % 2], xs.at[h], xr.at[o % 2],
               peers[h][1], peers[h][0])
        for h in range(2)
    ]

    def stage6(w):
        j = WAVES[w]

        @pl.when(owner_of(w) == a)
        def _():
            same, other = arrive()
            out_ref[place(c), :] = same
            out_ref[place(1 - c), :] = other
            if j >= 2:
                acc[place(c), :] = same
                acc[place(1 - c), :] = other
                for copy in outgoing:
                    copy.start()

    stages = (stage1, stage2, stage3, stage4, stage5, stage6)
    count = len(WAVES)
    for t in range(count + len(stages) - 1):
        for n, stage in enumerate(stages):
            if 0 <= t - n < count:
                stage(t - n)

    direct = owner_of(0) == a
    for w in range(1, count):
        direct = jnp.logical_or(direct, owner_of(w) == a)
    sent = jnp.logical_and(direct, mirrored)

    @pl.when(jnp.logical_not(direct))
    def _():
        for h in range(2):
            remote(acc.at[:, pl.ds(0, half_cols)], mirror.at[h], xs.at[h], xr.at[h], a, o).wait_recv()
        across = mirror[...].reshape(4 * rows, half_cols).T

        @pl.when(o % 2 == 0)
        def _():
            out_ref[...] = across[: 2 * rows]

        @pl.when(o % 2 == 1)
        def _():
            out_ref[...] = across[half_cols - 2 * rows :]

    for copy in started:
        copy.wait_send()
    for w in range(count):

        @pl.when(owner_of(w) != a)
        def _():
            to_owner[w].wait_send()

    @pl.when(sent)
    def _():
        for copy in outgoing:
            copy.wait_send()


def cube(half, metric, survive):
    aux_local, occ_local, ao = half.shape
    blocks_ao = survive.shape[2]
    gate = jnp.repeat(survive.reshape(blocks_ao).astype(jnp.bfloat16), ao // blocks_ao)
    blocks = (half * gate).transpose(1, 0, 2)
    naux = 8 * aux_local
    part = occ_local // 4
    depth = part * naux
    rows, cols = ao // 32, ao // 8
    waves = len(WAVES)
    dma, vmem = pltpu.SemaphoreType.DMA, pltpu.VMEM
    bf16 = jnp.bfloat16
    return pl.pallas_call(
        cube_kernel,
        out_shape=jax.ShapeDtypeStruct((2 * rows, cols), F32),
        in_specs=[pl.BlockSpec(memory_space=pltpu.VMEM)] * 2,
        out_specs=pl.BlockSpec(memory_space=pltpu.VMEM),
        scratch_shapes=[
            vmem((part, naux, ao), bf16),
            vmem((2, part // 2, aux_local, ao), bf16),
            vmem((naux, naux), bf16),
            vmem((depth, ao), bf16),
            vmem((ao // 4, depth), bf16),
            vmem((4, 4 * rows, depth), bf16),
            vmem((waves, 16, rows, cols), F32),
            vmem((waves, 16, rows, cols), bf16),
            vmem((waves, 4, rows, cols), bf16),
            vmem((waves, 4, rows, cols), bf16),
            vmem((waves, 2, 4, rows, cols), bf16),
            vmem((waves, 4, rows, cols), F32),
            vmem((waves, 3, rows, cols), bf16),
            vmem((waves, 2, rows // 2, cols), bf16),
            vmem((waves, 2, rows, cols), bf16),
            vmem((waves, rows, cols), F32),
            vmem((8, rows, cols), F32),
            vmem((2 * rows, cols), F32),
            vmem((2, 2 * rows, 2 * cols // 3), F32),
        ]
        + [dma((8,))] * 2
        + [dma((4, 2))] * 6
        + [dma((13,))] * 2
        + [dma((waves, 4))] * 2
        + [dma((waves, 8))] * 2
        + [dma((waves, 2))] * 4
        + [dma((waves,)), dma((8,)), dma((2,)), dma((2,))],
        compiler_params=pltpu.CompilerParams(
            collective_id=0, has_side_effects=True, vmem_limit_bytes=66 * 1000 * 1000
        ),
    )(blocks, metric)


def solution(mesh):
    full = mesh.shape["aux"] == 8 and mesh.shape["orb"] == 16
    return jax.shard_map(
        cube if full else plain,
        mesh=mesh,
        in_specs=(P("aux", "orb", None), P("aux", None), P("aux", "orb", None)),
        out_specs=P("orb", "aux"),
        check_vma=False,
    )
```

```python
import functools

import jax
import jax.numpy as jnp
from jax import lax
from jax.experimental import pallas as pl
from jax.experimental.pallas import tpu as pltpu
from jax.sharding import PartitionSpec as P

MESH = pl.DeviceIdType.MESH
F32 = jnp.float32


def gated(half, survive):
    aux_local, occ_local, ao_count = half.shape
    blocks_aux, blocks_occ, blocks_ao = survive.shape
    gate = survive.astype(jnp.bfloat16)
    shaped = half.reshape(
        blocks_aux, aux_local, blocks_occ, occ_local // blocks_occ, blocks_ao, ao_count // blocks_ao
    )
    return (shaped * gate[:, None, :, None, :, None]).reshape(aux_local, occ_local, ao_count)


def plain(half, metric, survive):
    aux_local, occ_local, ao_count = half.shape
    portion = lax.all_gather(gated(half, survive), "aux", axis=0, tiled=True)
    fit_total = jnp.dot(metric, portion.reshape(portion.shape[0], -1), preferred_element_type=F32)
    fitted = fit_total.astype(jnp.bfloat16).reshape(aux_local, occ_local, ao_count)
    group_width = ao_count // lax.axis_size("orb")
    row_start = lax.axis_index("orb") * group_width
    flat_rows = lax.all_gather(fitted, "orb", axis=1, tiled=True).reshape(-1, ao_count)
    left_rows = lax.dynamic_slice_in_dim(flat_rows, row_start, group_width, 1)
    partial_k = lax.dot_general(
        left_rows, flat_rows, (((0,), (0,)), ((), ())), preferred_element_type=F32
    )
    return lax.psum_scatter(partial_k, "aux", scatter_dimension=1, tiled=True)


WAVES = (
    (0, 0, 0), (0, 1, 0), (0, 2, 1), (1, 3, 0), (0, 0, 1), (1, 1, 0), (2, 2, 2), (1, 3, 1), (1, 0, 1),
)
EARLY = 2
CODES = 32767.0


def side(kind, half_of_x):
    return half_of_x if kind == 2 else kind


def block_at(x, side_of):
    return 2 * x + (x + side_of) % 2


def encode(tile, codes, scale):
    size = jnp.abs(tile)
    lanes = scale.shape[1]
    parts = tile.shape[1] // lanes
    peak = functools.reduce(jnp.maximum, [size[:, n * lanes : (n + 1) * lanes] for n in range(parts)])
    peak = jnp.maximum(jnp.max(peak, axis=0, keepdims=True), 1e-30)
    scale[...] = peak * (1.0 / CODES)
    grow = jnp.concatenate([CODES / peak] * parts, axis=1)
    codes[...] = jnp.round(tile * grow).astype(jnp.int32).astype(codes.dtype)


def decode(codes, scale):
    parts = codes.shape[1] // scale.shape[1]
    grow = jnp.concatenate([scale[...]] * parts, axis=1)
    return codes[...].astype(jnp.int32).astype(F32) * grow


def cube_kernel(
    half_ref, metric_ref, survive_ref, out_ref, raw, pick, blocks, held, via, whole, fit, turned, left,
    kf, q1, c1, far1, cf1, p1, cp1, v, q3, c3, far2, cf2, q4, c4, p2, cp2, ks, fin, acc, mirror,
    ins, ms, mr, zfs, zfr, zns, znr, zrs, zrr, ds, dr, f1s, f1r, p1s, p1r, f2s, f2r, p2s, p2r, zs, zr, xs, xr,
):
    a, o = lax.axis_index("aux"), lax.axis_index("orb")
    z, c = a // 2, a % 2
    x, y = o // 4, o % 4
    ao = fit.shape[1]
    n_own, part = blocks.shape[1], blocks.shape[0] // 4
    cut = part // 2
    naux = whole.shape[0]
    chunk, cols, rows = ao // 4, ao // 8, ao // 32
    split = rows // 2
    f_step, s_step = 4 - 3 * c, 1 + 3 * c
    f = x * (1 - c) + y * c
    s = y * (1 - c) + x * c
    partner = a + 1 - 2 * c

    def at_block(p):
        return pl.ds(p * cols, cols) if isinstance(p, int) else pl.ds(pl.multiple_of(p * cols, cols), cols)

    loads = []
    for p in range(8):
        load = pltpu.make_async_copy(
            half_ref.at[:, at_block(block_at(p % 4, p // 4))], raw.at[:, at_block(p)], ins.at[p]
        )
        load.start()
        loads.append(load)

    def orb_at(df, dsec):
        return ((f + df) % 4) * f_step + ((s + dsec) % 4) * s_step

    def aux_at(dz):
        return ((z + dz) % 4) * 2 + c

    mirrored = o // 2 != a
    peers = [(2 * a + h, o // 2) for h in range(2)]
    barrier = pltpu.get_barrier_semaphore()

    def greet(there_a, there_o):
        pl.semaphore_signal(barrier, inc=1, device_id={"aux": there_a, "orb": there_o}, device_id_type=MESH)

    for d in range(1, 8):
        greet((a + d) % 8, o)
    for d in (1, 3):
        greet(a, orb_at(d, 0))
        greet(a, orb_at(0, d))

    @pl.when(mirrored)
    def _():
        for to_o, to_a in peers:
            greet(to_a, to_o)

    def remote(src, dst, send, recv, to_a, to_o):
        return pltpu.make_async_remote_copy(
            src_ref=src, dst_ref=dst, send_sem=send, recv_sem=recv,
            device_id={"aux": to_a, "orb": to_o}, device_id_type=MESH,
        )

    started = []

    def go(copy):
        copy.start()
        started.append(copy)
        return copy

    depth = raw.shape[0]
    orbs = blocks.shape[0]
    row_of = lax.broadcasted_iota(jnp.int32, (depth, depth), 0)
    col_of = lax.broadcasted_iota(jnp.int32, (depth, depth), 1)
    wanted = lax.rem(row_of, n_own) * orbs + lax.div(row_of, n_own)
    pick[...] = jnp.where(wanted == col_of, 1.0, 0.0).astype(pick.dtype)

    def prepare(k):
        for p in (2 * k, 2 * k + 1):
            loads[p].wait()
            block = block_at(p % 4, p // 4)
            ordered = jnp.dot(pick[...], raw[:, at_block(p)], preferred_element_type=F32)
            for n in range(cols // 128):
                gate = survive_ref[0, block * (cols // 128) + n].astype(F32)
                kept = ordered[:, n * 128 : (n + 1) * 128] * gate
                blocks[:, :, pl.ds(p * cols + n * 128, 128)] = kept.astype(blocks.dtype).reshape(orbs, n_own, 128)

    def aux_rows(aux):
        return pl.ds(pl.multiple_of(aux * n_own, n_own), n_own)

    mine = aux_rows(a)
    span = [pl.ds(k * chunk, chunk) for k in range(4)]

    def orbitals(dz, first, count):
        return pl.ds(((z + dz) % 4) * part + first, count)

    far, near, relay, to_partner = {}, {}, {}, {}

    def issue(k):
        far[k] = [
            go(remote(blocks.at[orbitals(2, 0, cut), :, span[k]], via.at[0, :, :, span[k]],
                      zfs.at[k, 0], zfr.at[k, 0], aux_at(1), o)),
            go(remote(blocks.at[orbitals(2, cut, cut), :, span[k]], via.at[1, :, :, span[k]],
                      zfs.at[k, 1], zfr.at[k, 1], aux_at(3), o)),
        ]
        near[k] = [
            go(remote(blocks.at[orbitals(dz, 0, part), :, span[k]], held.at[:, mine, span[k]],
                      zns.at[k, n], znr.at[k, n], aux_at(dz), o))
            for n, dz in enumerate((1, 3))
        ]
        own = blocks.at[orbitals(0, 0, part), :, span[k]]
        to_partner[k, 3] = go(remote(own, held.at[:, mine, span[k]], ds.at[4 * k + 3], dr.at[4 * k + 3], partner, o))
        held[:, mine, span[k]] = own[...]

    prepare(0)
    pl.semaphore_wait(barrier, 11 + 2 * jnp.where(mirrored, 1, 0))
    issue(0)
    gather = [
        go(remote(metric_ref, whole.at[mine], ms.at[d], mr.at[d], (a + d) % 8, o)) for d in range(1, 8)
    ]
    whole[mine, :] = metric_ref[...]
    prepare(1)
    issue(1)
    prepare(2)
    prepare(3)

    def hand_over(k, n, dz):
        there = held.at[:, aux_rows(aux_at(dz)), span[k]]
        to_partner[k, n] = go(remote(there, there, ds.at[4 * k + n], dr.at[4 * k + n], partner, o))

    def finish(k):
        for copy in relay[k]:
            copy.wait_recv()
        hand_over(k, 2, 2)
        if k == 0:
            for copy in gather:
                copy.wait_recv()
        for n in range(4):
            to_partner[k, n].wait_recv()

        @pl.loop(0, part)
        def _(i):
            at = pl.ds(pl.multiple_of(i * naux, naux), naux)
            fit[at, span[k]] = jnp.dot(
                whole[...], held[i, :, span[k]], preferred_element_type=F32
            ).astype(fit.dtype)

        @pl.loop(0, chunk // 128)
        def _(t):
            at = pl.ds(pl.multiple_of(t * 128, 128), 128)
            src = pl.ds(pl.multiple_of(k * chunk + t * 128, 128), 128)
            turned[at, :] = fit[:, src].T

        for n in range(4):
            at = pl.ds(pl.multiple_of((2 * n + c) * rows, rows), rows)
            left[2 * k + n // 2, (n % 2) * rows : (n % 2 + 1) * rows, :] = turned[at, :]

    def pass_on(k):
        for copy in far[k]:
            copy.wait_recv()
        relay[k] = [
            go(remote(via.at[0, :, :, span[k]], held.at[pl.ds(0, cut), aux_rows(aux_at(3)), span[k]],
                      zrs.at[k, 0], zrr.at[k, 0], aux_at(1), o)),
            go(remote(via.at[1, :, :, span[k]], held.at[pl.ds(cut, cut), aux_rows(aux_at(1)), span[k]],
                      zrs.at[k, 1], zrr.at[k, 1], aux_at(3), o)),
        ]
        if k + 2 < 4:
            issue(k + 2)
        for copy in near[k]:
            copy.wait_recv()
        hand_over(k, 0, 3)
        hand_over(k, 1, 1)

    def target(w, dest, u):
        kind = WAVES[w][0]
        by_x = 2 * ((dest % 2 + side(kind, dest // 2)) % 2) + u
        by_y = 2 * u + (dest // 2 + side(kind, u)) % 2
        return by_x * (1 - c) + by_y * c

    def tile_of(w, df, u):
        dest = (f + df) % 4
        return (2 * dest + u) * (1 - c) + (2 * target(w, dest, u) + dest % 2) * c

    def turn(w, u):
        return (target(w, f, u) + 4 - s) % 4

    def multiply(w):
        rk, step, ck = WAVES[w]

        @pl.loop(0, 4)
        def _(g):
            p = 4 * side(rk, g // 2) + g
            q = 4 * side(ck, g // 2) + (g + step) % 4
            more = jnp.dot(left[p], fit[:, at_block(q)], preferred_element_type=F32)
            kf[w, 2 * g] = more[:rows]
            kf[w, 2 * g + 1] = more[rows:]

    def both(src, src_scale, dst, dst_scale, send, recv, to_o):
        return [
            remote(src, dst, send.at[0], recv.at[0], a, to_o),
            remote(src_scale, dst_scale, send.at[1], recv.at[1], a, to_o),
        ]

    first_far, first_in, second_far, second_in, to_owner = {}, {}, {}, {}, {}

    def ring_send(w, n, u, up):
        d = 0 if up else 1
        first_in[w, u, d] = [go(copy) for copy in both(
            q1.at[w, n], c1.at[w, n], p1.at[w, u, d], cp1.at[w, u, d], p1s.at[w, u, d], p1r.at[w, u, d],
            orb_at(1 if up else 3, 0),
        )]

    def stage1(w):
        multiply(w)
        for u, up in ((0, True), (1, False)):
            encode(kf[w, tile_of(w, 2, u)], q1.at[w, u], c1.at[w, u])
            first_far[w, u] = [go(copy) for copy in both(
                q1.at[w, u], c1.at[w, u], far1.at[w, u], cf1.at[w, u], f1s.at[w, u], f1r.at[w, u],
                orb_at(1 if up else 3, 0),
            )]
        for u, up in ((1, True), (0, False)):
            encode(kf[w, tile_of(w, 1 if up else 3, u)], q1.at[w, 2 + u], c1.at[w, 2 + u])
            ring_send(w, 2 + u, u, up)

    def stage2(w):
        for u, up in ((0, True), (1, False)):
            for copy in first_far[w, u]:
                copy.wait_recv()
            encode(
                kf[w, tile_of(w, 1 if up else 3, u)] + decode(far1.at[w, u], cf1.at[w, u]),
                q1.at[w, 4 + u], c1.at[w, 4 + u],
            )
            ring_send(w, 4 + u, u, up)

    def stage3(w):
        for u in range(2):
            total = kf[w, tile_of(w, 0, u)]
            for d in range(2):
                for copy in first_in[w, u, d]:
                    copy.wait_recv()
                total = total + decode(p1.at[w, u, d], cp1.at[w, u, d])
            v[w, u] = total
            second_far[w, u] = [
                both(
                    q3.at[w, u, pl.ds(d * split, split)], c3.at[w, u], far2.at[w, u], cf2.at[w, u],
                    f2s.at[w, u, d], f2r.at[w, u], orb_at(0, 1 + 2 * d),
                )
                for d in range(2)
            ]

            @pl.when(turn(w, u) == 2)
            def _():
                encode(total, q3.at[w, u], c3.at[w, u])
                for pair in second_far[w, u]:
                    for copy in pair:
                        copy.start()

    def stage4(w):
        for u in range(2):
            r = turn(w, u)
            late = jnp.where(r == 3, 1, 0)
            second_in[w, u] = both(
                q4.at[w, u], c4.at[w, u], p2.at[w, u, late], cp2.at[w, u, late],
                p2s.at[w, u], p2r.at[w, u, late], orb_at(0, r),
            )

            @pl.when(r % 2 == 1)
            def _():
                for copy in second_far[w, u][0]:
                    copy.wait_recv()
                at = pl.ds(pl.multiple_of(late * split, split), split)
                v[w, u, at] += decode(far2.at[w, u], cf2.at[w, u])
                encode(v[w, u], q4.at[w, u], c4.at[w, u])
                for copy in second_in[w, u]:
                    copy.start()

    def owner_of(w):
        step, ck = WAVES[w][1:]
        there = (x + step) % 4
        return 2 * there + (there + side(ck, x // 2)) % 2

    own_side = (x + y // 2) % 2

    def owned(w):
        return jnp.logical_and(own_side == side(WAVES[w][0], x // 2), owner_of(w) == a)

    def stage5(w):
        owner = owner_of(w)
        d = (owner + 8 - a) % 8
        to_owner[w] = remote(ks.at[w], fin.at[d], zs.at[w], zr.at[d], owner, o)
        for u in range(2):

            @pl.when(turn(w, u) == 0)
            def _():
                total = v[w, u]
                for n in range(2):
                    for copy in both(
                        q4.at[w, u], c4.at[w, u], p2.at[w, u, n], cp2.at[w, u, n], p2s.at[w, u], p2r.at[w, u, n], o
                    ):
                        copy.wait_recv()
                    total = total + decode(p2.at[w, u, n], cp2.at[w, u, n])
                ks[w] = total

                @pl.when(owner != a)
                def _():
                    to_owner[w].start()

                @pl.when(owner == a)
                def _():
                    fin[0] = total

    half_cols = 2 * cols // 3

    def place(c_rows):
        return pl.ds(pl.multiple_of(c_rows * rows, rows), rows)

    outgoing = [
        remote(acc.at[:, pl.ds(h * (cols - half_cols), half_cols)], mirror.at[o % 2], xs.at[h], xr.at[o % 2],
               peers[h][1], peers[h][0])
        for h in range(2)
    ]

    def stage6(w):
        @pl.when(owned(w))
        def _():
            for d in range(1, 8):
                remote(ks.at[0], fin.at[d], zs.at[0], zr.at[d], a, o).wait_recv()
            same = fin[0] + fin[2] + fin[4] + fin[6]
            other = fin[1] + fin[3] + fin[5] + fin[7]
            out_ref[place(c), :] = same
            out_ref[place(1 - c), :] = other
            if WAVES[w][1] or WAVES[w][0] != WAVES[w][2]:
                acc[place(c), :] = same
                acc[place(1 - c), :] = other
                for copy in outgoing:
                    copy.start()

    stages = (stage1, stage2, stage3, stage4, stage5, stage6)
    count = len(WAVES)

    for k in range(3):
        pass_on(k)
        if k:
            finish(k - 1)
    for w in range(EARLY):
        stage1(w)
    pass_on(3)
    for w in range(EARLY):
        stage2(w)
    finish(2)
    for w in range(EARLY):
        stage3(w)
    finish(3)
    for t in range(EARLY, count + len(stages) - 1):
        for n, stage in enumerate(stages):
            w = t - n
            if 0 <= w < count and (w >= EARLY or n > 2):
                stage(w)

    direct = functools.reduce(jnp.logical_or, [owned(w) for w in range(count)])

    @pl.when(jnp.logical_not(direct))
    def _():
        for h in range(2):
            remote(acc.at[:, pl.ds(0, half_cols)], mirror.at[h], xs.at[h], xr.at[h], a, o).wait_recv()
        across = mirror[...].reshape(4 * rows, half_cols).T

        @pl.when(o % 2 == 0)
        def _():
            out_ref[...] = across[: 2 * rows]

        @pl.when(o % 2 == 1)
        def _():
            out_ref[...] = across[half_cols - 2 * rows :]

    for copy in started:
        copy.wait_send()
    for w in range(count):
        for u in range(2):
            r = turn(w, u)

            @pl.when(r == 2)
            def _():
                for pair in second_far[w, u]:
                    for copy in pair:
                        copy.wait_send()

            @pl.when(r % 2 == 1)
            def _():
                for copy in second_in[w, u]:
                    copy.wait_send()

            @pl.when(jnp.logical_and(r == 0, owner_of(w) != a))
            def _():
                to_owner[w].wait_send()

    @pl.when(jnp.logical_and(direct, mirrored))
    def _():
        for copy in outgoing:
            copy.wait_send()


def cube(half, metric, survive):
    aux_local, occ_local, ao = half.shape
    naux = 8 * aux_local
    part = occ_local // 4
    depth = part * naux
    own = aux_local * occ_local
    rows, cols = ao // 32, ao // 8
    n = len(WAVES)
    dma, vmem = pltpu.SemaphoreType.DMA, pltpu.VMEM
    bf16, i16 = jnp.bfloat16, jnp.int16

    def coded(*lead, height=rows):
        return [vmem((*lead, height, cols), i16), vmem((*lead, 1, 128), F32)]

    return pl.pallas_call(
        cube_kernel,
        out_shape=jax.ShapeDtypeStruct((2 * rows, cols), F32),
        in_specs=[
            pl.BlockSpec(memory_space=pl.ANY),
            pl.BlockSpec(memory_space=pltpu.VMEM),
            pl.BlockSpec(memory_space=pltpu.SMEM),
        ],
        out_specs=pl.BlockSpec(memory_space=pltpu.VMEM),
        scratch_shapes=[
            vmem((own, ao), bf16),
            vmem((own, own), bf16),
            vmem((occ_local, aux_local, ao), bf16),
            vmem((part, naux, ao), bf16),
            vmem((2, part // 2, aux_local, ao), bf16),
            vmem((naux, naux), bf16),
            vmem((depth, ao), bf16),
            vmem((ao // 4, depth), bf16),
            vmem((8, 2 * rows, depth), bf16),
            vmem((n, 8, rows, cols), F32),
            *coded(n, 6),
            *coded(n, 2),
            *coded(n, 2, 2),
            vmem((n, 2, rows, cols), F32),
            *coded(n, 2),
            *coded(n, 2, height=rows // 2),
            *coded(n, 2),
            *coded(n, 2, 2),
            vmem((n, rows, cols), F32),
            vmem((8, rows, cols), F32),
            vmem((2 * rows, cols), F32),
            vmem((2, 2 * rows, 2 * cols // 3), F32),
        ]
        + [dma((8,))] * 3
        + [dma((4, 2))] * 6
        + [dma((16,))] * 2
        + [dma((n, 2, 2))] * 2
        + [dma((n, 2, 2, 2))] * 2
        + [dma((n, 2, 2, 2)), dma((n, 2, 2))]
        + [dma((n, 2, 2)), dma((n, 2, 2, 2))]
        + [dma((n,)), dma((8,)), dma((2,)), dma((2,))],
        compiler_params=pltpu.CompilerParams(
            collective_id=0, has_side_effects=True, vmem_limit_bytes=66 * 1000 * 1000
        ),
    )(half.reshape(own, ao), metric, survive.reshape(1, -1))


def solution(mesh):
    full = mesh.shape["aux"] == 8 and mesh.shape["orb"] == 16
    return jax.shard_map(
        cube if full else plain,
        mesh=mesh,
        in_specs=(P("aux", "orb", None), P("aux", None), P("aux", "orb", None)),
        out_specs=P("orb", "aux"),
        check_vma=False,
    )
```

```python
import functools

import jax
import jax.numpy as jnp
from jax import lax
from jax.experimental import pallas as pl
from jax.experimental.pallas import tpu as pltpu
from jax.sharding import PartitionSpec as P

MESH = pl.DeviceIdType.MESH
F32 = jnp.float32


def gated(half, survive):
    aux_local, occ_local, ao_count = half.shape
    blocks_aux, blocks_occ, blocks_ao = survive.shape
    gate = survive.astype(jnp.bfloat16)
    shaped = half.reshape(
        blocks_aux, aux_local, blocks_occ, occ_local // blocks_occ, blocks_ao, ao_count // blocks_ao
    )
    return (shaped * gate[:, None, :, None, :, None]).reshape(aux_local, occ_local, ao_count)


def plain(half, metric, survive):
    aux_local, occ_local, ao_count = half.shape
    portion = lax.all_gather(gated(half, survive), "aux", axis=0, tiled=True)
    fit_total = jnp.dot(metric, portion.reshape(portion.shape[0], -1), preferred_element_type=F32)
    fitted = fit_total.astype(jnp.bfloat16).reshape(aux_local, occ_local, ao_count)
    group_width = ao_count // lax.axis_size("orb")
    row_start = lax.axis_index("orb") * group_width
    flat_rows = lax.all_gather(fitted, "orb", axis=1, tiled=True).reshape(-1, ao_count)
    left_rows = lax.dynamic_slice_in_dim(flat_rows, row_start, group_width, 1)
    partial_k = lax.dot_general(
        left_rows, flat_rows, (((0,), (0,)), ((), ())), preferred_element_type=F32
    )
    return lax.psum_scatter(partial_k, "aux", scatter_dimension=1, tiled=True)


WAVES = (
    (0, 0, 0), (0, 1, 0), (0, 2, 1), (1, 3, 0), (0, 0, 1), (1, 1, 0), (2, 2, 2), (1, 3, 1), (1, 0, 1),
)
EARLY = 2
LAGS = (0, 4, 7, 9, 11, 13)
CODES = 32767.0


def side(kind, half_of_x):
    return half_of_x if kind == 2 else kind


def block_at(x, side_of):
    return 2 * x + (x + side_of) % 2


def encode(tile, codes, scale):
    size = jnp.abs(tile)
    lanes = scale.shape[1]
    parts = tile.shape[1] // lanes
    peak = functools.reduce(jnp.maximum, [size[:, n * lanes : (n + 1) * lanes] for n in range(parts)])
    peak = jnp.maximum(jnp.max(peak, axis=0, keepdims=True), 1e-30)
    scale[...] = peak * (1.0 / CODES)
    grow = jnp.concatenate([CODES / peak] * parts, axis=1)
    codes[...] = jnp.round(tile * grow).astype(jnp.int32).astype(codes.dtype)


def decode(codes, scale):
    parts = codes.shape[1] // scale.shape[1]
    grow = jnp.concatenate([scale[...]] * parts, axis=1)
    return codes[...].astype(jnp.int32).astype(F32) * grow


def cube_kernel(
    half_ref, metric_ref, survive_ref, out_ref, raw, pick, blocks, held, via, whole, fit, turned, left,
    kf, q1, c1, far1, cf1, p1, cp1, v, q3, c3, far2, cf2, q4, c4, p2, cp2, ks, cks, fin, cfin, kept, acc, cacc, mirror,
    cmirror,
    ins, ms, mr, zfs, zfr, zns, znr, zrs, zrr, ds, dr, f1s, f1r, p1s, p1r, f2s, f2r, p2s, p2r, zs, zr, xs, xr,
):
    a, o = lax.axis_index("aux"), lax.axis_index("orb")
    z, c = a // 2, a % 2
    x, y = o // 4, o % 4
    ao = fit.shape[1]
    n_own, part = blocks.shape[1], blocks.shape[0] // 4
    cut = part // 2
    naux = whole.shape[0]
    chunk, cols, rows = ao // 4, ao // 8, ao // 32
    split = rows // 2
    f_step, s_step = 4 - 3 * c, 1 + 3 * c
    f = x * (1 - c) + y * c
    s = y * (1 - c) + x * c
    partner = a + 1 - 2 * c

    def at_block(p):
        return pl.ds(p * cols, cols) if isinstance(p, int) else pl.ds(pl.multiple_of(p * cols, cols), cols)

    loads = []
    for p in range(8):
        load = pltpu.make_async_copy(
            half_ref.at[:, at_block(block_at(p % 4, p // 4))], raw.at[:, at_block(p)], ins.at[p]
        )
        load.start()
        loads.append(load)

    def orb_at(df, dsec):
        return ((f + df) % 4) * f_step + ((s + dsec) % 4) * s_step

    def aux_at(dz):
        return ((z + dz) % 4) * 2 + c

    mirrored = o // 2 != a
    peers = [(2 * a + h, o // 2) for h in range(2)]
    barrier = pltpu.get_barrier_semaphore()

    def greet(there_a, there_o):
        pl.semaphore_signal(barrier, inc=1, device_id={"aux": there_a, "orb": there_o}, device_id_type=MESH)

    for d in range(1, 8):
        greet((a + d) % 8, o)
    for d in (1, 3):
        greet(a, orb_at(d, 0))
        greet(a, orb_at(0, d))

    def remote(src, dst, send, recv, to_a, to_o):
        return pltpu.make_async_remote_copy(
            src_ref=src, dst_ref=dst, send_sem=send, recv_sem=recv,
            device_id={"aux": to_a, "orb": to_o}, device_id_type=MESH,
        )

    started = []

    def go(copy):
        copy.start()
        started.append(copy)
        return copy

    depth = raw.shape[0]
    orbs = blocks.shape[0]
    row_of = lax.broadcasted_iota(jnp.int32, (depth, depth), 0)
    col_of = lax.broadcasted_iota(jnp.int32, (depth, depth), 1)
    wanted = lax.rem(row_of, n_own) * orbs + lax.div(row_of, n_own)
    pick[...] = jnp.where(wanted == col_of, 1.0, 0.0).astype(pick.dtype)

    def prepare(k):
        for p in (2 * k, 2 * k + 1):
            loads[p].wait()
            block = block_at(p % 4, p // 4)
            ordered = jnp.dot(pick[...], raw[:, at_block(p)], preferred_element_type=F32)
            for n in range(cols // 128):
                gate = survive_ref[0, block * (cols // 128) + n].astype(F32)
                kept = ordered[:, n * 128 : (n + 1) * 128] * gate
                blocks[:, :, pl.ds(p * cols + n * 128, 128)] = kept.astype(blocks.dtype).reshape(orbs, n_own, 128)

    def aux_rows(aux):
        return pl.ds(pl.multiple_of(aux * n_own, n_own), n_own)

    mine = aux_rows(a)
    span = [pl.ds(k * chunk, chunk) for k in range(4)]

    def orbitals(dz, first, count):
        return pl.ds(((z + dz) % 4) * part + first, count)

    far, near, relay, to_partner = {}, {}, {}, {}

    def issue(k):
        far[k] = [
            go(remote(blocks.at[orbitals(2, 0, cut), :, span[k]], via.at[0, :, :, span[k]],
                      zfs.at[k, 0], zfr.at[k, 0], aux_at(1), o)),
            go(remote(blocks.at[orbitals(2, cut, cut), :, span[k]], via.at[1, :, :, span[k]],
                      zfs.at[k, 1], zfr.at[k, 1], aux_at(3), o)),
        ]
        near[k] = [
            go(remote(blocks.at[orbitals(dz, 0, part), :, span[k]], held.at[:, mine, span[k]],
                      zns.at[k, n], znr.at[k, n], aux_at(dz), o))
            for n, dz in enumerate((1, 3))
        ]
        own = blocks.at[orbitals(0, 0, part), :, span[k]]
        to_partner[k, 3] = go(remote(own, held.at[:, mine, span[k]], ds.at[4 * k + 3], dr.at[4 * k + 3], partner, o))
        held[:, mine, span[k]] = own[...]

    prepare(0)
    pl.semaphore_wait(barrier, 11)
    issue(0)
    gather = [
        go(remote(metric_ref, whole.at[mine], ms.at[d], mr.at[d], (a + d) % 8, o)) for d in range(1, 8)
    ]
    whole[mine, :] = metric_ref[...]
    prepare(1)
    issue(1)
    prepare(2)
    prepare(3)

    def hand_over(k, n, dz):
        there = held.at[:, aux_rows(aux_at(dz)), span[k]]
        to_partner[k, n] = go(remote(there, there, ds.at[4 * k + n], dr.at[4 * k + n], partner, o))

    def finish(k):
        for copy in relay[k]:
            copy.wait_recv()
        hand_over(k, 2, 2)
        if k == 0:
            for copy in gather:
                copy.wait_recv()
        for n in range(4):
            to_partner[k, n].wait_recv()

        @pl.loop(0, part)
        def _(i):
            at = pl.ds(pl.multiple_of(i * naux, naux), naux)
            fit[at, span[k]] = jnp.dot(
                whole[...], held[i, :, span[k]], preferred_element_type=F32
            ).astype(fit.dtype)

        @pl.loop(0, chunk // 128)
        def _(t):
            at = pl.ds(pl.multiple_of(t * 128, 128), 128)
            src = pl.ds(pl.multiple_of(k * chunk + t * 128, 128), 128)
            turned[at, :] = fit[:, src].T

        for n in range(4):
            at = pl.ds(pl.multiple_of((2 * n + c) * rows, rows), rows)
            left[2 * k + n // 2, (n % 2) * rows : (n % 2 + 1) * rows, :] = turned[at, :]

    def pass_on(k):
        for copy in far[k]:
            copy.wait_recv()
        relay[k] = [
            go(remote(via.at[0, :, :, span[k]], held.at[pl.ds(0, cut), aux_rows(aux_at(3)), span[k]],
                      zrs.at[k, 0], zrr.at[k, 0], aux_at(1), o)),
            go(remote(via.at[1, :, :, span[k]], held.at[pl.ds(cut, cut), aux_rows(aux_at(1)), span[k]],
                      zrs.at[k, 1], zrr.at[k, 1], aux_at(3), o)),
        ]
        if k + 2 < 4:
            issue(k + 2)
        for copy in near[k]:
            copy.wait_recv()
        hand_over(k, 0, 3)
        hand_over(k, 1, 1)

    def target(w, dest, u):
        kind = WAVES[w][0]
        by_x = 2 * ((dest % 2 + side(kind, dest // 2)) % 2) + u
        by_y = 2 * u + (dest // 2 + side(kind, u)) % 2
        return by_x * (1 - c) + by_y * c

    def tile_of(w, df, u):
        dest = (f + df) % 4
        return (2 * dest + u) * (1 - c) + (2 * target(w, dest, u) + dest % 2) * c

    def turn(w, u):
        return (target(w, f, u) + 4 - s) % 4

    def multiply(w):
        rk, step, ck = WAVES[w]

        @pl.loop(0, 4)
        def _(g):
            p = 4 * side(rk, g // 2) + g
            q = 4 * side(ck, g // 2) + (g + step) % 4
            more = jnp.dot(left[p], fit[:, at_block(q)], preferred_element_type=F32)
            kf[w, 2 * g] = more[:rows]
            kf[w, 2 * g + 1] = more[rows:]

    def both(src, src_scale, dst, dst_scale, send, recv, to_o):
        return [
            remote(src, dst, send.at[0], recv.at[0], a, to_o),
            remote(src_scale, dst_scale, send.at[1], recv.at[1], a, to_o),
        ]

    first_far, first_in, second_far, second_in, to_owner = {}, {}, {}, {}, {}

    def ring_send(w, n, u, up):
        d = 0 if up else 1
        first_in[w, u, d] = [go(copy) for copy in both(
            q1.at[w, n], c1.at[w, n], p1.at[w, u, d], cp1.at[w, u, d], p1s.at[w, u, d], p1r.at[w, u, d],
            orb_at(1 if up else 3, 0),
        )]

    def stage1(w):
        multiply(w)
        for u, up in ((0, True), (1, False)):
            encode(kf[w, tile_of(w, 2, u)], q1.at[w, u], c1.at[w, u])
            first_far[w, u] = [go(copy) for copy in both(
                q1.at[w, u], c1.at[w, u], far1.at[w, u], cf1.at[w, u], f1s.at[w, u], f1r.at[w, u],
                orb_at(1 if up else 3, 0),
            )]
        for u, up in ((1, True), (0, False)):
            encode(kf[w, tile_of(w, 1 if up else 3, u)], q1.at[w, 2 + u], c1.at[w, 2 + u])
            ring_send(w, 2 + u, u, up)

    def stage2(w):
        for u, up in ((0, True), (1, False)):
            for copy in first_far[w, u]:
                copy.wait_recv()
            encode(
                kf[w, tile_of(w, 1 if up else 3, u)] + decode(far1.at[w, u], cf1.at[w, u]),
                q1.at[w, 4 + u], c1.at[w, 4 + u],
            )
            ring_send(w, 4 + u, u, up)

    def stage3(w):
        for u in range(2):
            total = kf[w, tile_of(w, 0, u)]
            for d in range(2):
                for copy in first_in[w, u, d]:
                    copy.wait_recv()
                total = total + decode(p1.at[w, u, d], cp1.at[w, u, d])
            v[w, u] = total
            second_far[w, u] = [
                both(
                    q3.at[w, u, pl.ds(d * split, split)], c3.at[w, u], far2.at[w, u], cf2.at[w, u],
                    f2s.at[w, u, d], f2r.at[w, u], orb_at(0, 1 + 2 * d),
                )
                for d in range(2)
            ]

            @pl.when(turn(w, u) == 2)
            def _():
                encode(total, q3.at[w, u], c3.at[w, u])
                for pair in second_far[w, u]:
                    for copy in pair:
                        copy.start()

    def stage4(w):
        for u in range(2):
            r = turn(w, u)
            late = jnp.where(r == 3, 1, 0)
            second_in[w, u] = both(
                q4.at[w, u], c4.at[w, u], p2.at[w, u, late], cp2.at[w, u, late],
                p2s.at[w, u], p2r.at[w, u, late], orb_at(0, r),
            )

            @pl.when(r % 2 == 1)
            def _():
                for copy in second_far[w, u][0]:
                    copy.wait_recv()
                at = pl.ds(pl.multiple_of(late * split, split), split)
                v[w, u, at] += decode(far2.at[w, u], cf2.at[w, u])
                encode(v[w, u], q4.at[w, u], c4.at[w, u])
                for copy in second_in[w, u]:
                    copy.start()

    def owner_of(w):
        step, ck = WAVES[w][1:]
        there = (x + step) % 4
        return 2 * there + (there + side(ck, x // 2)) % 2

    own_side = (x + y // 2) % 2

    def owned(w):
        return jnp.logical_and(own_side == side(WAVES[w][0], x // 2), owner_of(w) == a)

    def stage5(w):
        owner = owner_of(w)
        d = (owner + 8 - a) % 8
        to_owner[w] = [
            remote(ks.at[w], fin.at[d], zs.at[w, 0], zr.at[d, 0], owner, o),
            remote(cks.at[w], cfin.at[d], zs.at[w, 1], zr.at[d, 1], owner, o),
        ]
        for u in range(2):

            @pl.when(turn(w, u) == 0)
            def _():
                total = v[w, u]
                for n in range(2):
                    for copy in both(
                        q4.at[w, u], c4.at[w, u], p2.at[w, u, n], cp2.at[w, u, n], p2s.at[w, u], p2r.at[w, u, n], o
                    ):
                        copy.wait_recv()
                    total = total + decode(p2.at[w, u, n], cp2.at[w, u, n])

                @pl.when(owner != a)
                def _():
                    encode(total, ks.at[w], cks.at[w])
                    for copy in to_owner[w]:
                        copy.start()

                @pl.when(owner == a)
                def _():
                    kept[...] = total

    half_cols = 2 * cols // 3

    def place(c_rows):
        return pl.ds(pl.multiple_of(c_rows * rows, rows), rows)

    outgoing = [
        [
            remote(acc.at[h], mirror.at[o % 2], xs.at[h, 0], xr.at[o % 2, 0], peers[h][1], peers[h][0]),
            remote(cacc.at[h], cmirror.at[o % 2], xs.at[h, 1], xr.at[o % 2, 1], peers[h][1], peers[h][0]),
        ]
        for h in range(2)
    ]

    def stage6(w):
        @pl.when(owned(w))
        def _():
            for d in range(1, 8):
                remote(ks.at[0], fin.at[d], zs.at[0, 0], zr.at[d, 0], a, o).wait_recv()
                remote(cks.at[0], cfin.at[d], zs.at[0, 1], zr.at[d, 1], a, o).wait_recv()
            part_of = [decode(fin.at[d], cfin.at[d]) for d in range(1, 8)]
            out_ref[place(c), :] = kept[...] + part_of[1] + part_of[3] + part_of[5]
            out_ref[place(1 - c), :] = part_of[0] + part_of[2] + part_of[4] + part_of[6]
            if WAVES[w][1] or WAVES[w][0] != WAVES[w][2]:
                for h in range(2):
                    encode(out_ref[:, h * (cols - half_cols) : h * (cols - half_cols) + half_cols], acc.at[h], cacc.at[h])
                for pair in outgoing:
                    for copy in pair:
                        copy.start()

    stages = (stage1, stage2, stage3, stage4, stage5, stage6)
    count = len(WAVES)

    for k in range(3):
        pass_on(k)
        if k:
            finish(k - 1)
    for w in range(EARLY):
        stage1(w)
    pass_on(3)
    for w in range(EARLY):
        stage2(w)
    finish(2)
    for w in range(EARLY):
        stage3(w)
    finish(3)
    for t in range(EARLY, count + LAGS[-1]):
        for n, stage in enumerate(stages):
            w = t - LAGS[n]
            if 0 <= w < count and (w >= EARLY or n > 2):
                stage(w)

    direct = functools.reduce(jnp.logical_or, [owned(w) for w in range(count)])

    @pl.when(jnp.logical_not(direct))
    def _():
        for h in range(2):
            remote(acc.at[h], mirror.at[h], xs.at[h, 0], xr.at[h, 0], a, o).wait_recv()
            remote(cacc.at[h], cmirror.at[h], xs.at[h, 1], xr.at[h, 1], a, o).wait_recv()
        across = jnp.concatenate([decode(mirror.at[h], cmirror.at[h]) for h in range(2)], axis=0).T

        @pl.when(o % 2 == 0)
        def _():
            out_ref[...] = across[: 2 * rows]

        @pl.when(o % 2 == 1)
        def _():
            out_ref[...] = across[half_cols - 2 * rows :]

    for copy in started:
        copy.wait_send()
    for w in range(count):
        for u in range(2):
            r = turn(w, u)

            @pl.when(r == 2)
            def _():
                for pair in second_far[w, u]:
                    for copy in pair:
                        copy.wait_send()

            @pl.when(r % 2 == 1)
            def _():
                for copy in second_in[w, u]:
                    copy.wait_send()

            @pl.when(jnp.logical_and(r == 0, owner_of(w) != a))
            def _():
                for copy in to_owner[w]:
                    copy.wait_send()

    @pl.when(jnp.logical_and(direct, mirrored))
    def _():
        for pair in outgoing:
            for copy in pair:
                copy.wait_send()


def cube(half, metric, survive):
    aux_local, occ_local, ao = half.shape
    naux = 8 * aux_local
    part = occ_local // 4
    depth = part * naux
    own = aux_local * occ_local
    rows, cols = ao // 32, ao // 8
    n = len(WAVES)
    dma, vmem = pltpu.SemaphoreType.DMA, pltpu.VMEM
    bf16, i16 = jnp.bfloat16, jnp.int16

    def coded(*lead, height=rows, width=cols):
        return [vmem((*lead, height, width), i16), vmem((*lead, 1, 128), F32)]

    return pl.pallas_call(
        cube_kernel,
        out_shape=jax.ShapeDtypeStruct((2 * rows, cols), F32),
        in_specs=[
            pl.BlockSpec(memory_space=pl.ANY),
            pl.BlockSpec(memory_space=pltpu.VMEM),
            pl.BlockSpec(memory_space=pltpu.SMEM),
        ],
        out_specs=pl.BlockSpec(memory_space=pltpu.VMEM),
        scratch_shapes=[
            vmem((own, ao), bf16),
            vmem((own, own), bf16),
            vmem((occ_local, aux_local, ao), bf16),
            vmem((part, naux, ao), bf16),
            vmem((2, part // 2, aux_local, ao), bf16),
            vmem((naux, naux), bf16),
            vmem((depth, ao), bf16),
            vmem((ao // 4, depth), bf16),
            vmem((8, 2 * rows, depth), bf16),
            vmem((n, 8, rows, cols), F32),
            *coded(n, 6),
            *coded(n, 2),
            *coded(n, 2, 2),
            vmem((n, 2, rows, cols), F32),
            *coded(n, 2),
            *coded(n, 2, height=rows // 2),
            *coded(n, 2),
            *coded(n, 2, 2),
            *coded(n),
            *coded(8),
            vmem((rows, cols), F32),
            *coded(2, height=2 * rows, width=2 * cols // 3),
            *coded(2, height=2 * rows, width=2 * cols // 3),
        ]
        + [dma((8,))] * 3
        + [dma((4, 2))] * 6
        + [dma((16,))] * 2
        + [dma((n, 2, 2))] * 2
        + [dma((n, 2, 2, 2))] * 2
        + [dma((n, 2, 2, 2)), dma((n, 2, 2))]
        + [dma((n, 2, 2)), dma((n, 2, 2, 2))]
        + [dma((n, 2)), dma((8, 2)), dma((2, 2)), dma((2, 2))],
        compiler_params=pltpu.CompilerParams(
            collective_id=0, has_side_effects=True, vmem_limit_bytes=66 * 1000 * 1000
        ),
    )(half.reshape(own, ao), metric, survive.reshape(1, -1))


def solution(mesh):
    full = mesh.shape["aux"] == 8 and mesh.shape["orb"] == 16
    return jax.shard_map(
        cube if full else plain,
        mesh=mesh,
        in_specs=(P("aux", "orb", None), P("aux", None), P("aux", "orb", None)),
        out_specs=P("orb", "aux"),
        check_vma=False,
    )
```

```python
import functools

import jax
import jax.numpy as jnp
from jax import lax
from jax.experimental import pallas as pl
from jax.experimental.pallas import tpu as pltpu
from jax.sharding import PartitionSpec as P

MESH = pl.DeviceIdType.MESH
F32 = jnp.float32


def gated(half, survive):
    aux_local, occ_local, ao_count = half.shape
    blocks_aux, blocks_occ, blocks_ao = survive.shape
    gate = survive.astype(jnp.bfloat16)
    shaped = half.reshape(
        blocks_aux, aux_local, blocks_occ, occ_local // blocks_occ, blocks_ao, ao_count // blocks_ao
    )
    return (shaped * gate[:, None, :, None, :, None]).reshape(aux_local, occ_local, ao_count)


def plain(half, metric, survive):
    aux_local, occ_local, ao_count = half.shape
    portion = lax.all_gather(gated(half, survive), "aux", axis=0, tiled=True)
    fit_total = jnp.dot(metric, portion.reshape(portion.shape[0], -1), preferred_element_type=F32)
    fitted = fit_total.astype(jnp.bfloat16).reshape(aux_local, occ_local, ao_count)
    group_width = ao_count // lax.axis_size("orb")
    row_start = lax.axis_index("orb") * group_width
    flat_rows = lax.all_gather(fitted, "orb", axis=1, tiled=True).reshape(-1, ao_count)
    left_rows = lax.dynamic_slice_in_dim(flat_rows, row_start, group_width, 1)
    partial_k = lax.dot_general(
        left_rows, flat_rows, (((0,), (0,)), ((), ())), preferred_element_type=F32
    )
    return lax.psum_scatter(partial_k, "aux", scatter_dimension=1, tiled=True)


WAVES = (
    (0, (0, 0), 0), (0, (1, 1), 0), (0, (0, 2), 1), (1, (3, 3), 0), (0, (2, 0), 1), (1, (1, 1), 0),
    (2, (2, 2), 2), (1, (3, 3), 1), (1, (0, 0), 1),
)
PLAN = (
    "r0", "n0", "r1", "n1", "g0", "r2", "q0", "n2", "g1", "r3", "q1", "a0", "n3", "a1",
    "g2", "g3", "q2", "a2", "b0", "b1", "q3", "a3", "a4", "a5", "b2", "c0", "a6", "b3",
    "c1", "a7", "b4", "c2", "d0", "a8", "b5", "c3", "d1", "b6", "c4", "d2", "e0", "b7",
    "c5", "d3", "e1", "b8", "c6", "d4", "e2", "f0", "c7", "d5", "e3", "f1", "c8", "d6",
    "e4", "f2", "d7", "e5", "f3", "d8", "e6", "f4", "e7", "f5", "e8", "f6", "f7", "f8",
)
CODES = 32767.0


def side(kind, half_of_x):
    return half_of_x if kind == 2 else kind


def block_at(x, side_of):
    return 2 * x + (x + side_of) % 2


def encode(tile, codes, scale):
    size = jnp.abs(tile)
    lanes = scale.shape[1]
    parts = tile.shape[1] // lanes
    peak = functools.reduce(jnp.maximum, [size[:, n * lanes : (n + 1) * lanes] for n in range(parts)])
    peak = jnp.maximum(jnp.max(peak, axis=0, keepdims=True), 1e-30)
    scale[...] = peak * (1.0 / CODES)
    grow = jnp.concatenate([CODES / peak] * parts, axis=1)
    codes[...] = jnp.round(tile * grow).astype(jnp.int32).astype(codes.dtype)


def decode(codes, scale):
    parts = codes.shape[1] // scale.shape[1]
    grow = jnp.concatenate([scale[...]] * parts, axis=1)
    return codes[...].astype(jnp.int32).astype(F32) * grow


def cube_kernel(
    half_ref, metric_ref, survive_ref, out_ref, raw, pick, blocks, held, via, whole, fit, turned, left,
    kf, q1, c1, far1, cf1, p1, cp1, v, q3, c3, far2, cf2, q4, c4, p2, cp2, ks, cks, fin, cfin, kept, acc, cacc, mirror,
    cmirror,
    ins, ms, mr, zfs, zfr, zns, znr, zrs, zrr, ds, dr, f1s, f1r, p1s, p1r, f2s, f2r, p2s, p2r, zs, zr, xs, xr,
):
    a, o = lax.axis_index("aux"), lax.axis_index("orb")
    z, c = a // 2, a % 2
    x, y = o // 4, o % 4
    ao = fit.shape[1]
    n_own, part = blocks.shape[1], blocks.shape[0] // 4
    cut = part // 2
    naux = whole.shape[0]
    chunk, cols, rows = ao // 4, ao // 8, ao // 32
    split = rows // 2
    f_step, s_step = 4 - 3 * c, 1 + 3 * c
    f = x * (1 - c) + y * c
    s = y * (1 - c) + x * c
    partner = a + 1 - 2 * c

    def at_block(p):
        return pl.ds(p * cols, cols) if isinstance(p, int) else pl.ds(pl.multiple_of(p * cols, cols), cols)

    loads = []
    for p in range(8):
        load = pltpu.make_async_copy(
            half_ref.at[:, at_block(block_at(p % 4, p // 4))], raw.at[:, at_block(p)], ins.at[p]
        )
        load.start()
        loads.append(load)

    def orb_at(df, dsec):
        return ((f + df) % 4) * f_step + ((s + dsec) % 4) * s_step

    def aux_at(dz):
        return ((z + dz) % 4) * 2 + c

    mirrored = o // 2 != a
    peers = [(2 * a + h, o // 2) for h in range(2)]
    barrier = pltpu.get_barrier_semaphore()

    def greet(there_a, there_o):
        pl.semaphore_signal(barrier, inc=1, device_id={"aux": there_a, "orb": there_o}, device_id_type=MESH)

    for d in range(1, 8):
        greet((a + d) % 8, o)
    for d in (1, 3):
        greet(a, orb_at(d, 0))
        greet(a, orb_at(0, d))

    def remote(src, dst, send, recv, to_a, to_o):
        return pltpu.make_async_remote_copy(
            src_ref=src, dst_ref=dst, send_sem=send, recv_sem=recv,
            device_id={"aux": to_a, "orb": to_o}, device_id_type=MESH,
        )

    started = []

    def go(copy):
        copy.start()
        started.append(copy)
        return copy

    depth = raw.shape[0]
    orbs = blocks.shape[0]
    row_of = lax.broadcasted_iota(jnp.int32, (depth, depth), 0)
    col_of = lax.broadcasted_iota(jnp.int32, (depth, depth), 1)
    wanted = lax.rem(row_of, n_own) * orbs + lax.div(row_of, n_own)
    pick[...] = jnp.where(wanted == col_of, 1.0, 0.0).astype(pick.dtype)

    def prepare(k):
        for p in (2 * k, 2 * k + 1):
            loads[p].wait()
            block = block_at(p % 4, p // 4)
            ordered = jnp.dot(pick[...], raw[:, at_block(p)], preferred_element_type=F32)
            for n in range(cols // 128):
                gate = survive_ref[0, block * (cols // 128) + n].astype(F32)
                kept = ordered[:, n * 128 : (n + 1) * 128] * gate
                blocks[:, :, pl.ds(p * cols + n * 128, 128)] = kept.astype(blocks.dtype).reshape(orbs, n_own, 128)

    def aux_rows(aux):
        return pl.ds(pl.multiple_of(aux * n_own, n_own), n_own)

    mine = aux_rows(a)
    span = [pl.ds(k * chunk, chunk) for k in range(4)]

    def orbitals(dz, first, count):
        return pl.ds(((z + dz) % 4) * part + first, count)

    far, near, relay, to_partner = {}, {}, {}, {}

    def issue(k):
        far[k] = [
            go(remote(blocks.at[orbitals(2, 0, cut), :, span[k]], via.at[0, :, :, span[k]],
                      zfs.at[k, 0], zfr.at[k, 0], aux_at(1), o)),
            go(remote(blocks.at[orbitals(2, cut, cut), :, span[k]], via.at[1, :, :, span[k]],
                      zfs.at[k, 1], zfr.at[k, 1], aux_at(3), o)),
        ]
        near[k] = [
            go(remote(blocks.at[orbitals(dz, 0, part), :, span[k]], held.at[:, mine, span[k]],
                      zns.at[k, n], znr.at[k, n], aux_at(dz), o))
            for n, dz in enumerate((1, 3))
        ]
        own = blocks.at[orbitals(0, 0, part), :, span[k]]
        to_partner[k, 3] = go(remote(own, held.at[:, mine, span[k]], ds.at[4 * k + 3], dr.at[4 * k + 3], partner, o))
        held[:, mine, span[k]] = own[...]

    prepare(0)
    pl.semaphore_wait(barrier, 11)
    issue(0)
    gather = [
        go(remote(metric_ref, whole.at[mine], ms.at[d], mr.at[d], (a + d) % 8, o)) for d in range(1, 8)
    ]
    whole[mine, :] = metric_ref[...]
    prepare(1)
    issue(1)
    prepare(2)
    prepare(3)

    def hand_over(k, n, dz):
        there = held.at[:, aux_rows(aux_at(dz)), span[k]]
        to_partner[k, n] = go(remote(there, there, ds.at[4 * k + n], dr.at[4 * k + n], partner, o))

    def gathered(k):
        for copy in relay[k]:
            copy.wait_recv()
        hand_over(k, 2, 2)

    def finish(k):
        if k == 0:
            for copy in gather:
                copy.wait_recv()
        for n in range(4):
            to_partner[k, n].wait_recv()

        for i in range(part):
            fit[i * naux : (i + 1) * naux, span[k]] = jnp.dot(
                whole[...], held[i, :, span[k]], preferred_element_type=F32
            ).astype(fit.dtype)
        for t in range(chunk // 128):
            turned[t * 128 : (t + 1) * 128, :] = fit[:, k * chunk + t * 128 : k * chunk + (t + 1) * 128].T

        for n in range(4):
            at = pl.ds(pl.multiple_of((2 * n + c) * rows, rows), rows)
            left[2 * k + n // 2, (n % 2) * rows : (n % 2 + 1) * rows, :] = turned[at, :]

    def pass_on(k):
        for copy in far[k]:
            copy.wait_recv()
        relay[k] = [
            go(remote(via.at[0, :, :, span[k]], held.at[pl.ds(0, cut), aux_rows(aux_at(3)), span[k]],
                      zrs.at[k, 0], zrr.at[k, 0], aux_at(1), o)),
            go(remote(via.at[1, :, :, span[k]], held.at[pl.ds(cut, cut), aux_rows(aux_at(1)), span[k]],
                      zrs.at[k, 1], zrr.at[k, 1], aux_at(3), o)),
        ]
        if k + 2 < 4:
            issue(k + 2)

    def take(k):
        for copy in near[k]:
            copy.wait_recv()
        hand_over(k, 0, 3)
        hand_over(k, 1, 1)

    def target(w, dest, u):
        kind = WAVES[w][0]
        by_x = 2 * ((dest % 2 + side(kind, dest // 2)) % 2) + u
        by_y = 2 * u + (dest // 2 + side(kind, u)) % 2
        return by_x * (1 - c) + by_y * c

    def tile_of(w, df, u):
        dest = (f + df) % 4
        return (2 * dest + u) * (1 - c) + (2 * target(w, dest, u) + dest % 2) * c

    def turn(w, u):
        return (target(w, f, u) + 4 - s) % 4

    def multiply(w):
        rk, step, ck = WAVES[w]

        @pl.loop(0, 4, unroll=True)
        def _(g):
            p = 4 * side(rk, g // 2) + g
            q = 4 * side(ck, g // 2) + (g + step[0] + (step[1] - step[0]) * (g // 2)) % 4
            more = jnp.dot(left[p], fit[:, at_block(q)], preferred_element_type=F32)
            kf[w, 2 * g] = more[:rows]
            kf[w, 2 * g + 1] = more[rows:]

    def both(src, src_scale, dst, dst_scale, send, recv, to_o):
        return [
            remote(src, dst, send.at[0], recv.at[0], a, to_o),
            remote(src_scale, dst_scale, send.at[1], recv.at[1], a, to_o),
        ]

    first_far, first_in, second_far, second_in, to_owner = {}, {}, {}, {}, {}

    def ring_send(w, n, u, up):
        d = 0 if up else 1
        first_in[w, u, d] = [go(copy) for copy in both(
            q1.at[w, n], c1.at[w, n], p1.at[w, u, d], cp1.at[w, u, d], p1s.at[w, u, d], p1r.at[w, u, d],
            orb_at(1 if up else 3, 0),
        )]

    def stage1(w):
        multiply(w)
        for u, up in ((0, True), (1, False)):
            encode(kf[w, tile_of(w, 2, u)], q1.at[w, u], c1.at[w, u])
            first_far[w, u] = [go(copy) for copy in both(
                q1.at[w, u], c1.at[w, u], far1.at[w, u], cf1.at[w, u], f1s.at[w, u], f1r.at[w, u],
                orb_at(1 if up else 3, 0),
            )]
        for u, up in ((1, True), (0, False)):
            encode(kf[w, tile_of(w, 1 if up else 3, u)], q1.at[w, 2 + u], c1.at[w, 2 + u])
            ring_send(w, 2 + u, u, up)

    def stage2(w):
        for u, up in ((0, True), (1, False)):
            for copy in first_far[w, u]:
                copy.wait_recv()
            encode(
                kf[w, tile_of(w, 1 if up else 3, u)] + decode(far1.at[w, u], cf1.at[w, u]),
                q1.at[w, 4 + u], c1.at[w, 4 + u],
            )
            ring_send(w, 4 + u, u, up)

    def stage3(w):
        for u in range(2):
            total = kf[w, tile_of(w, 0, u)]
            for d in range(2):
                for copy in first_in[w, u, d]:
                    copy.wait_recv()
                total = total + decode(p1.at[w, u, d], cp1.at[w, u, d])
            v[w, u] = total
            second_far[w, u] = [
                both(
                    q3.at[w, u, pl.ds(d * split, split)], c3.at[w, u], far2.at[w, u], cf2.at[w, u],
                    f2s.at[w, u, d], f2r.at[w, u], orb_at(0, 1 + 2 * d),
                )
                for d in range(2)
            ]

            @pl.when(turn(w, u) == 2)
            def _():
                encode(total, q3.at[w, u], c3.at[w, u])
                for pair in second_far[w, u]:
                    for copy in pair:
                        copy.start()

    def stage4(w):
        for u in range(2):
            r = turn(w, u)
            late = jnp.where(r == 3, 1, 0)
            second_in[w, u] = both(
                q4.at[w, u], c4.at[w, u], p2.at[w, u, late], cp2.at[w, u, late],
                p2s.at[w, u], p2r.at[w, u, late], orb_at(0, r),
            )

            @pl.when(r % 2 == 1)
            def _():
                for copy in second_far[w, u][0]:
                    copy.wait_recv()
                at = pl.ds(pl.multiple_of(late * split, split), split)
                v[w, u, at] += decode(far2.at[w, u], cf2.at[w, u])
                encode(v[w, u], q4.at[w, u], c4.at[w, u])
                for copy in second_in[w, u]:
                    copy.start()

    def owner_of(w):
        step, ck = WAVES[w][1:]
        there = (x + step[0] + (step[1] - step[0]) * (x // 2)) % 4
        return 2 * there + (there + side(ck, x // 2)) % 2

    own_side = (x + y // 2) % 2

    def owned(w):
        return jnp.logical_and(own_side == side(WAVES[w][0], x // 2), owner_of(w) == a)

    def stage5(w):
        owner = owner_of(w)
        d = (owner + 8 - a) % 8
        to_owner[w] = [
            remote(ks.at[w], fin.at[d], zs.at[w, 0], zr.at[d, 0], owner, o),
            remote(cks.at[w], cfin.at[d], zs.at[w, 1], zr.at[d, 1], owner, o),
        ]
        for u in range(2):

            @pl.when(turn(w, u) == 0)
            def _():
                total = v[w, u]
                for n in range(2):
                    for copy in both(
                        q4.at[w, u], c4.at[w, u], p2.at[w, u, n], cp2.at[w, u, n], p2s.at[w, u], p2r.at[w, u, n], o
                    ):
                        copy.wait_recv()
                    total = total + decode(p2.at[w, u, n], cp2.at[w, u, n])

                @pl.when(owner != a)
                def _():
                    encode(total, ks.at[w], cks.at[w])
                    for copy in to_owner[w]:
                        copy.start()

                @pl.when(owner == a)
                def _():
                    kept[...] = total

    half_cols = 2 * cols // 3

    def place(c_rows):
        return pl.ds(pl.multiple_of(c_rows * rows, rows), rows)

    outgoing = [
        [
            remote(acc.at[h], mirror.at[o % 2], xs.at[h, 0], xr.at[o % 2, 0], peers[h][1], peers[h][0]),
            remote(cacc.at[h], cmirror.at[o % 2], xs.at[h, 1], xr.at[o % 2, 1], peers[h][1], peers[h][0]),
        ]
        for h in range(2)
    ]

    def stage6(w):
        @pl.when(owned(w))
        def _():
            for d in range(1, 8):
                remote(ks.at[0], fin.at[d], zs.at[0, 0], zr.at[d, 0], a, o).wait_recv()
                remote(cks.at[0], cfin.at[d], zs.at[0, 1], zr.at[d, 1], a, o).wait_recv()
            part_of = [decode(fin.at[d], cfin.at[d]) for d in range(1, 8)]
            out_ref[place(c), :] = kept[...] + part_of[1] + part_of[3] + part_of[5]
            out_ref[place(1 - c), :] = part_of[0] + part_of[2] + part_of[4] + part_of[6]
            if sum(WAVES[w][1]) or WAVES[w][0] != WAVES[w][2]:
                for h in range(2):
                    encode(out_ref[:, h * (cols - half_cols) : h * (cols - half_cols) + half_cols], acc.at[h], cacc.at[h])
                for pair in outgoing:
                    for copy in pair:
                        copy.start()

    count = len(WAVES)

    calls = dict(
        r=pass_on, n=take, g=gathered, q=finish, a=stage1, b=stage2, c=stage3, d=stage4, e=stage5, f=stage6
    )
    for name in PLAN:
        calls[name[0]](int(name[1]))
    direct = functools.reduce(jnp.logical_or, [owned(w) for w in range(count)])

    @pl.when(jnp.logical_not(direct))
    def _():
        for h in range(2):
            remote(acc.at[h], mirror.at[h], xs.at[h, 0], xr.at[h, 0], a, o).wait_recv()
            remote(cacc.at[h], cmirror.at[h], xs.at[h, 1], xr.at[h, 1], a, o).wait_recv()
        across = jnp.concatenate([decode(mirror.at[h], cmirror.at[h]) for h in range(2)], axis=0).T

        @pl.when(o % 2 == 0)
        def _():
            out_ref[...] = across[: 2 * rows]

        @pl.when(o % 2 == 1)
        def _():
            out_ref[...] = across[half_cols - 2 * rows :]

    for copy in started:
        copy.wait_send()
    for w in range(count):
        for u in range(2):
            r = turn(w, u)

            @pl.when(r == 2)
            def _():
                for pair in second_far[w, u]:
                    for copy in pair:
                        copy.wait_send()

            @pl.when(r % 2 == 1)
            def _():
                for copy in second_in[w, u]:
                    copy.wait_send()

            @pl.when(jnp.logical_and(r == 0, owner_of(w) != a))
            def _():
                for copy in to_owner[w]:
                    copy.wait_send()

    @pl.when(jnp.logical_and(direct, mirrored))
    def _():
        for pair in outgoing:
            for copy in pair:
                copy.wait_send()


def cube(half, metric, survive):
    aux_local, occ_local, ao = half.shape
    naux = 8 * aux_local
    part = occ_local // 4
    depth = part * naux
    own = aux_local * occ_local
    rows, cols = ao // 32, ao // 8
    n = len(WAVES)
    dma, vmem = pltpu.SemaphoreType.DMA, pltpu.VMEM
    bf16, i16 = jnp.bfloat16, jnp.int16

    def coded(*lead, height=rows, width=cols):
        return [vmem((*lead, height, width), i16), vmem((*lead, 1, 128), F32)]

    return pl.pallas_call(
        cube_kernel,
        out_shape=jax.ShapeDtypeStruct((2 * rows, cols), F32),
        in_specs=[
            pl.BlockSpec(memory_space=pl.ANY),
            pl.BlockSpec(memory_space=pltpu.VMEM),
            pl.BlockSpec(memory_space=pltpu.SMEM),
        ],
        out_specs=pl.BlockSpec(memory_space=pltpu.VMEM),
        scratch_shapes=[
            vmem((own, ao), bf16),
            vmem((own, own), bf16),
            vmem((occ_local, aux_local, ao), bf16),
            vmem((part, naux, ao), bf16),
            vmem((2, part // 2, aux_local, ao), bf16),
            vmem((naux, naux), bf16),
            vmem((depth, ao), bf16),
            vmem((ao // 4, depth), bf16),
            vmem((8, 2 * rows, depth), bf16),
            vmem((n, 8, rows, cols), F32),
            *coded(n, 6),
            *coded(n, 2),
            *coded(n, 2, 2),
            vmem((n, 2, rows, cols), F32),
            *coded(n, 2),
            *coded(n, 2, height=rows // 2),
            *coded(n, 2),
            *coded(n, 2, 2),
            *coded(n),
            *coded(8),
            vmem((rows, cols), F32),
            *coded(2, height=2 * rows, width=2 * cols // 3),
            *coded(2, height=2 * rows, width=2 * cols // 3),
        ]
        + [dma((8,))] * 3
        + [dma((4, 2))] * 6
        + [dma((16,))] * 2
        + [dma((n, 2, 2))] * 2
        + [dma((n, 2, 2, 2))] * 2
        + [dma((n, 2, 2, 2)), dma((n, 2, 2))]
        + [dma((n, 2, 2)), dma((n, 2, 2, 2))]
        + [dma((n, 2)), dma((8, 2)), dma((2, 2)), dma((2, 2))],
        compiler_params=pltpu.CompilerParams(
            collective_id=0, has_side_effects=True, vmem_limit_bytes=66 * 1000 * 1000
        ),
    )(half.reshape(own, ao), metric, survive.reshape(1, -1))


def solution(mesh):
    full = mesh.shape["aux"] == 8 and mesh.shape["orb"] == 16
    return jax.shard_map(
        cube if full else plain,
        mesh=mesh,
        in_specs=(P("aux", "orb", None), P("aux", None), P("aux", "orb", None)),
        out_specs=P("orb", "aux"),
        check_vma=False,
    )
```

```python
import functools

import jax
import jax.numpy as jnp
from jax import lax
from jax.experimental import pallas as pl
from jax.experimental.pallas import tpu as pltpu
from jax.sharding import PartitionSpec as P

MESH = pl.DeviceIdType.MESH
F32 = jnp.float32


def gated(half, survive):
    aux_local, occ_local, ao_count = half.shape
    blocks_aux, blocks_occ, blocks_ao = survive.shape
    gate = survive.astype(jnp.bfloat16)
    shaped = half.reshape(
        blocks_aux, aux_local, blocks_occ, occ_local // blocks_occ, blocks_ao, ao_count // blocks_ao
    )
    return (shaped * gate[:, None, :, None, :, None]).reshape(aux_local, occ_local, ao_count)


def plain(half, metric, survive):
    aux_local, occ_local, ao_count = half.shape
    portion = lax.all_gather(gated(half, survive), "aux", axis=0, tiled=True)
    fit_total = jnp.dot(metric, portion.reshape(portion.shape[0], -1), preferred_element_type=F32)
    fitted = fit_total.astype(jnp.bfloat16).reshape(aux_local, occ_local, ao_count)
    group_width = ao_count // lax.axis_size("orb")
    row_start = lax.axis_index("orb") * group_width
    flat_rows = lax.all_gather(fitted, "orb", axis=1, tiled=True).reshape(-1, ao_count)
    left_rows = lax.dynamic_slice_in_dim(flat_rows, row_start, group_width, 1)
    partial_k = lax.dot_general(
        left_rows, flat_rows, (((0,), (0,)), ((), ())), preferred_element_type=F32
    )
    return lax.psum_scatter(partial_k, "aux", scatter_dimension=1, tiled=True)


WAVES = (
    (0, (0, 0), 0), (0, (1, 1), 0), (0, (0, 2), 1), (1, (3, 3), 0), (0, (2, 0), 1),
    (1, (1, 1), 0), (2, (2, 2), 2), (1, (3, 3), 1), (1, (0, 0), 1),
)
PLAN = (
    "r0", "n0", "r1", "n1", "g0", "r2", "q0", "n2", "g1", "r3", "q1", "a0", "n3", "a1",
    "g2", "g3", "q2", "a2", "b0", "b1", "q3", "a3", "a4", "a5", "b2", "c0", "a6", "b3",
    "c1", "a7", "b4", "c2", "d0", "a8", "b5", "c3", "d1", "b6", "c4", "d2", "e0", "b7",
    "c5", "d3", "e1", "b8", "c6", "d4", "e2", "f0", "c7", "d5", "e3", "f1", "c8", "d6",
    "e4", "f2", "d7", "e5", "f3", "d8", "e6", "f4", "e7", "f5", "e8", "f6", "f7", "f8",
)
CODES = 32767.0


def side(kind, half_of_x):
    return half_of_x if kind == 2 else kind


def block_at(x, side_of):
    return 2 * x + (x + side_of) % 2


def encode(tile, codes, scale):
    size = jnp.abs(tile)
    lanes = scale.shape[1]
    parts = tile.shape[1] // lanes
    peak = functools.reduce(jnp.maximum, [size[:, n * lanes : (n + 1) * lanes] for n in range(parts)])
    peak = jnp.maximum(jnp.max(peak, axis=0, keepdims=True), 1e-30)
    scale[...] = peak * (1.0 / CODES)
    grow = jnp.concatenate([CODES / peak] * parts, axis=1)
    codes[...] = jnp.round(tile * grow).astype(jnp.int32).astype(codes.dtype)


def decode(codes, scale):
    parts = codes.shape[1] // scale.shape[1]
    grow = jnp.concatenate([scale[...]] * parts, axis=1)
    return codes[...].astype(jnp.int32).astype(F32) * grow


def cube_kernel(
    half_ref, metric_ref, survive_ref, out_ref, raw, pick, blocks, held, via, whole, fit, turned, left,
    kf, q1, c1, far1, cf1, p1, cp1, v, q3, c3, far2, cf2, q4, c4, p2, cp2, ks, cks, fin, cfin, kept, acc, cacc, mirror,
    cmirror,
    ins, bulk, mr, zfr, znr, zrr, dr, f1r, p1r, f2s, f2r, p2s, p2r, zs, zr, xs, xr,
):
    a, o = lax.axis_index("aux"), lax.axis_index("orb")
    z, c = a // 2, a % 2
    x, y = o // 4, o % 4
    ao = fit.shape[1]
    n_own, part = blocks.shape[1], blocks.shape[0] // 4
    cut = part // 2
    naux = whole.shape[0]
    chunk, cols, rows = ao // 4, ao // 8, ao // 32
    split = rows // 2
    f_step, s_step = 4 - 3 * c, 1 + 3 * c
    f = x * (1 - c) + y * c
    s = y * (1 - c) + x * c
    partner = a + 1 - 2 * c

    def at_block(p):
        return pl.ds(p * cols, cols) if isinstance(p, int) else pl.ds(pl.multiple_of(p * cols, cols), cols)

    loads = []
    for p in range(8):
        load = pltpu.make_async_copy(
            half_ref.at[:, at_block(block_at(p % 4, p // 4))], raw.at[:, at_block(p)], ins.at[p]
        )
        load.start()
        loads.append(load)

    def orb_at(df, dsec):
        return ((f + df) % 4) * f_step + ((s + dsec) % 4) * s_step

    def aux_at(dz):
        return ((z + dz) % 4) * 2 + c

    mirrored = o // 2 != a
    peers = [(2 * a + h, o // 2) for h in range(2)]
    barrier = pltpu.get_barrier_semaphore()

    def greet(there_a, there_o):
        pl.semaphore_signal(barrier, inc=1, device_id={"aux": there_a, "orb": there_o}, device_id_type=MESH)

    for d in range(1, 8):
        greet((a + d) % 8, o)
    for d in (1, 3):
        greet(a, orb_at(d, 0))
        greet(a, orb_at(0, d))

    def remote(src, dst, send, recv, to_a, to_o):
        return pltpu.make_async_remote_copy(
            src_ref=src, dst_ref=dst, send_sem=send, recv_sem=recv,
            device_id={"aux": to_a, "orb": to_o}, device_id_type=MESH,
        )

    def go(copy):
        copy.start()
        return copy

    depth = raw.shape[0]
    orbs = blocks.shape[0]
    row_of = lax.broadcasted_iota(jnp.int32, (depth, depth), 0)
    col_of = lax.broadcasted_iota(jnp.int32, (depth, depth), 1)
    wanted = lax.rem(row_of, n_own) * orbs + lax.div(row_of, n_own)
    pick[...] = jnp.where(wanted == col_of, 1.0, 0.0).astype(pick.dtype)

    def prepare(k):
        for p in (2 * k, 2 * k + 1):
            loads[p].wait()
            block = block_at(p % 4, p // 4)
            ordered = jnp.dot(pick[...], raw[:, at_block(p)], preferred_element_type=F32)
            for n in range(cols // 128):
                gate = survive_ref[0, block * (cols // 128) + n].astype(F32)
                kept = ordered[:, n * 128 : (n + 1) * 128] * gate
                blocks[:, :, pl.ds(p * cols + n * 128, 128)] = kept.astype(blocks.dtype).reshape(orbs, n_own, 128)

    def aux_rows(aux):
        return pl.ds(pl.multiple_of(aux * n_own, n_own), n_own)

    mine = aux_rows(a)
    span = [pl.ds(k * chunk, chunk) for k in range(4)]

    def orbitals(dz, first, count):
        return pl.ds(((z + dz) % 4) * part + first, count)

    far, near, relay, to_partner = {}, {}, {}, {}

    def issue(k):
        far[k] = [
            go(remote(blocks.at[orbitals(2, 0, cut), :, span[k]], via.at[0, :, :, span[k]],
                      bulk.at[0], zfr.at[k, 0], aux_at(1), o)),
            go(remote(blocks.at[orbitals(2, cut, cut), :, span[k]], via.at[1, :, :, span[k]],
                      bulk.at[0], zfr.at[k, 1], aux_at(3), o)),
        ]
        near[k] = [
            go(remote(blocks.at[orbitals(dz, 0, part), :, span[k]], held.at[:, mine, span[k]],
                      bulk.at[0], znr.at[k, n], aux_at(dz), o))
            for n, dz in enumerate((1, 3))
        ]
        own = blocks.at[orbitals(0, 0, part), :, span[k]]
        to_partner[k, 3] = go(remote(own, held.at[:, mine, span[k]], bulk.at[0], dr.at[4 * k + 3], partner, o))
        held[:, mine, span[k]] = own[...]

    prepare(0)
    pl.semaphore_wait(barrier, 11)
    issue(0)
    gather = [
        go(remote(metric_ref, whole.at[mine], bulk.at[3], mr.at[d], (a + d) % 8, o)) for d in range(1, 8)
    ]
    whole[mine, :] = metric_ref[...]
    prepare(1)
    issue(1)
    prepare(2)
    prepare(3)

    def hand_over(k, n, dz):
        there = held.at[:, aux_rows(aux_at(dz)), span[k]]
        to_partner[k, n] = go(remote(there, there, bulk.at[2], dr.at[4 * k + n], partner, o))

    def gathered(k):
        for copy in relay[k]:
            copy.wait_recv()
        hand_over(k, 2, 2)

    def finish(k):
        if k == 0:
            for copy in gather:
                copy.wait_recv()
        for n in range(4):
            to_partner[k, n].wait_recv()

        for i in range(part):
            fit[i * naux : (i + 1) * naux, span[k]] = jnp.dot(
                whole[...], held[i, :, span[k]], preferred_element_type=F32
            ).astype(fit.dtype)
        for t in range(chunk // 128):
            turned[t * 128 : (t + 1) * 128, :] = fit[:, k * chunk + t * 128 : k * chunk + (t + 1) * 128].T

        for n in range(4):
            at = pl.ds(pl.multiple_of((2 * n + c) * rows, rows), rows)
            left[2 * k + n // 2, (n % 2) * rows : (n % 2 + 1) * rows, :] = turned[at, :]

    def pass_on(k):
        for copy in far[k]:
            copy.wait_recv()
        relay[k] = [
            go(remote(via.at[0, :, :, span[k]], held.at[pl.ds(0, cut), aux_rows(aux_at(3)), span[k]],
                      bulk.at[1], zrr.at[k, 0], aux_at(1), o)),
            go(remote(via.at[1, :, :, span[k]], held.at[pl.ds(cut, cut), aux_rows(aux_at(1)), span[k]],
                      bulk.at[1], zrr.at[k, 1], aux_at(3), o)),
        ]
        if k + 2 < 4:
            issue(k + 2)

    def take(k):
        for copy in near[k]:
            copy.wait_recv()
        hand_over(k, 0, 3)
        hand_over(k, 1, 1)

    def target(w, dest, u):
        kind = WAVES[w][0]
        by_x = 2 * ((dest % 2 + side(kind, dest // 2)) % 2) + u
        by_y = 2 * u + (dest // 2 + side(kind, u)) % 2
        return by_x * (1 - c) + by_y * c

    def tile_of(w, df, u):
        dest = (f + df) % 4
        return (2 * dest + u) * (1 - c) + (2 * target(w, dest, u) + dest % 2) * c

    def turn(w, u):
        return (target(w, f, u) + 4 - s) % 4

    def multiply(w):
        rk, step, ck = WAVES[w]

        @pl.loop(0, 4, unroll=True)
        def _(g):
            p = 4 * side(rk, g // 2) + g
            q = 4 * side(ck, g // 2) + (g + step[0] + (step[1] - step[0]) * (g // 2)) % 4
            more = jnp.dot(left[p], fit[:, at_block(q)], preferred_element_type=F32)
            kf[w, 2 * g] = more[:rows]
            kf[w, 2 * g + 1] = more[rows:]

    def both(src, src_scale, dst, dst_scale, send, recv, to_o):
        return [
            remote(src, dst, send[0], recv.at[0], a, to_o),
            remote(src_scale, dst_scale, send[1], recv.at[1], a, to_o),
        ]

    first_far, first_in, second_far, second_in, to_owner = {}, {}, {}, {}, {}

    def ring_send(w, n, u, up):
        d = 0 if up else 1
        first_in[w, u, d] = [go(copy) for copy in both(
            q1.at[w, n], c1.at[w, n], p1.at[w, u, d], cp1.at[w, u, d], (bulk.at[4], bulk.at[5]), p1r.at[w, u, d],
            orb_at(1 if up else 3, 0),
        )]

    def stage1(w):
        multiply(w)
        for u, up in ((0, True), (1, False)):
            encode(kf[w, tile_of(w, 2, u)], q1.at[w, u], c1.at[w, u])
            first_far[w, u] = [go(copy) for copy in both(
                q1.at[w, u], c1.at[w, u], far1.at[w, u], cf1.at[w, u], (bulk.at[4], bulk.at[5]), f1r.at[w, u],
                orb_at(1 if up else 3, 0),
            )]
        for u, up in ((1, True), (0, False)):
            encode(kf[w, tile_of(w, 1 if up else 3, u)], q1.at[w, 2 + u], c1.at[w, 2 + u])
            ring_send(w, 2 + u, u, up)

    def stage2(w):
        for u, up in ((0, True), (1, False)):
            for copy in first_far[w, u]:
                copy.wait_recv()
            encode(
                kf[w, tile_of(w, 1 if up else 3, u)] + decode(far1.at[w, u], cf1.at[w, u]),
                q1.at[w, 4 + u], c1.at[w, 4 + u],
            )
            ring_send(w, 4 + u, u, up)

    def stage3(w):
        for u in range(2):
            total = kf[w, tile_of(w, 0, u)]
            for d in range(2):
                for copy in first_in[w, u, d]:
                    copy.wait_recv()
                total = total + decode(p1.at[w, u, d], cp1.at[w, u, d])
            v[w, u] = total
            second_far[w, u] = [
                both(
                    q3.at[w, u, pl.ds(d * split, split)], c3.at[w, u], far2.at[w, u], cf2.at[w, u],
                    (f2s.at[w, u, 0, d], f2s.at[w, u, 1, d]), f2r.at[w, u], orb_at(0, 1 + 2 * d),
                )
                for d in range(2)
            ]

            @pl.when(turn(w, u) == 2)
            def _():
                encode(total, q3.at[w, u], c3.at[w, u])
                for pair in second_far[w, u]:
                    for copy in pair:
                        copy.start()

    def stage4(w):
        for u in range(2):
            r = turn(w, u)
            late = jnp.where(r == 3, 1, 0)
            second_in[w, u] = both(
                q4.at[w, u], c4.at[w, u], p2.at[w, u, late], cp2.at[w, u, late],
                (p2s.at[w, u, 0], p2s.at[w, u, 1]), p2r.at[w, u, late], orb_at(0, r),
            )

            @pl.when(r % 2 == 1)
            def _():
                for copy in second_far[w, u][0]:
                    copy.wait_recv()
                at = pl.ds(pl.multiple_of(late * split, split), split)
                v[w, u, at] += decode(far2.at[w, u], cf2.at[w, u])
                encode(v[w, u], q4.at[w, u], c4.at[w, u])
                for copy in second_in[w, u]:
                    copy.start()

    def owner_of(w):
        step, ck = WAVES[w][1:]
        there = (x + step[0] + (step[1] - step[0]) * (x // 2)) % 4
        return 2 * there + (there + side(ck, x // 2)) % 2

    own_side = (x + y // 2) % 2

    def owned(w):
        return jnp.logical_and(own_side == side(WAVES[w][0], x // 2), owner_of(w) == a)

    def stage5(w):
        owner = owner_of(w)
        d = (owner + 8 - a) % 8
        to_owner[w] = [
            remote(ks.at[w], fin.at[d], zs.at[w, 0], zr.at[d, 0], owner, o),
            remote(cks.at[w], cfin.at[d], zs.at[w, 1], zr.at[d, 1], owner, o),
        ]
        for u in range(2):

            @pl.when(turn(w, u) == 0)
            def _():
                total = v[w, u]
                for n in range(2):
                    for copy in both(
                        q4.at[w, u], c4.at[w, u], p2.at[w, u, n], cp2.at[w, u, n], (p2s.at[w, u, 0], p2s.at[w, u, 1]), p2r.at[w, u, n], o
                    ):
                        copy.wait_recv()
                    total = total + decode(p2.at[w, u, n], cp2.at[w, u, n])

                @pl.when(owner != a)
                def _():
                    encode(total, ks.at[w], cks.at[w])
                    for copy in to_owner[w]:
                        copy.start()

                @pl.when(owner == a)
                def _():
                    kept[...] = total

    half_cols = 2 * cols // 3

    def place(c_rows):
        return pl.ds(pl.multiple_of(c_rows * rows, rows), rows)

    outgoing = [
        [
            remote(acc.at[h], mirror.at[o % 2], xs.at[h, 0], xr.at[o % 2, 0], peers[h][1], peers[h][0]),
            remote(cacc.at[h], cmirror.at[o % 2], xs.at[h, 1], xr.at[o % 2, 1], peers[h][1], peers[h][0]),
        ]
        for h in range(2)
    ]

    def stage6(w):
        for u in range(2):
            r = turn(w, u)

            @pl.when(r == 2)
            def _():
                for pair in second_far[w, u]:
                    for copy in pair:
                        copy.wait_send()

            @pl.when(r % 2 == 1)
            def _():
                for copy in second_in[w, u]:
                    copy.wait_send()

        @pl.when(owned(w))
        def _():
            for d in range(1, 8):
                remote(ks.at[0], fin.at[d], zs.at[0, 0], zr.at[d, 0], a, o).wait_recv()
                remote(cks.at[0], cfin.at[d], zs.at[0, 1], zr.at[d, 1], a, o).wait_recv()
            part_of = [decode(fin.at[d], cfin.at[d]) for d in range(1, 8)]
            out_ref[place(c), :] = kept[...] + part_of[1] + part_of[3] + part_of[5]
            out_ref[place(1 - c), :] = part_of[0] + part_of[2] + part_of[4] + part_of[6]
            if sum(WAVES[w][1]) or WAVES[w][0] != WAVES[w][2]:
                for h in range(2):
                    encode(out_ref[:, h * (cols - half_cols) : h * (cols - half_cols) + half_cols], acc.at[h], cacc.at[h])
                for pair in outgoing:
                    for copy in pair:
                        copy.start()

    count = len(WAVES)

    calls = dict(
        r=pass_on, n=take, g=gathered, q=finish, a=stage1, b=stage2, c=stage3, d=stage4, e=stage5, f=stage6
    )
    for name in PLAN:
        calls[name[0]](int(name[1]))
    direct = functools.reduce(jnp.logical_or, [owned(w) for w in range(count)])

    sent = (blocks, via, held.at[:, pl.ds(0, 3 * n_own)], whole.at[pl.ds(0, 7 * n_own)], q1, c1)
    for n, ref in enumerate(sent):
        remote(ref, ref, bulk.at[n], xr.at[0, 0], a, o).wait_send()
    for w in range(count):

        @pl.when(jnp.logical_and(jnp.logical_or(turn(w, 0) == 0, turn(w, 1) == 0), owner_of(w) != a))
        def _():
            for copy in to_owner[w]:
                copy.wait_send()

    @pl.when(jnp.logical_not(direct))
    def _():
        for h in range(2):
            remote(acc.at[h], mirror.at[h], xs.at[h, 0], xr.at[h, 0], a, o).wait_recv()
            remote(cacc.at[h], cmirror.at[h], xs.at[h, 1], xr.at[h, 1], a, o).wait_recv()
        across = jnp.concatenate([decode(mirror.at[h], cmirror.at[h]) for h in range(2)], axis=0).T

        @pl.when(o % 2 == 0)
        def _():
            out_ref[...] = across[: 2 * rows]

        @pl.when(o % 2 == 1)
        def _():
            out_ref[...] = across[half_cols - 2 * rows :]

    @pl.when(jnp.logical_and(direct, mirrored))
    def _():
        for pair in outgoing:
            for copy in pair:
                copy.wait_send()


def cube(half, metric, survive):
    aux_local, occ_local, ao = half.shape
    naux = 8 * aux_local
    part = occ_local // 4
    depth = part * naux
    own = aux_local * occ_local
    rows, cols = ao // 32, ao // 8
    n = len(WAVES)
    dma, vmem = pltpu.SemaphoreType.DMA, pltpu.VMEM
    bf16, i16 = jnp.bfloat16, jnp.int16

    def coded(*lead, height=rows, width=cols):
        return [vmem((*lead, height, width), i16), vmem((*lead, 1, 128), F32)]

    return pl.pallas_call(
        cube_kernel,
        out_shape=jax.ShapeDtypeStruct((2 * rows, cols), F32),
        in_specs=[
            pl.BlockSpec(memory_space=pl.ANY),
            pl.BlockSpec(memory_space=pltpu.VMEM),
            pl.BlockSpec(memory_space=pltpu.SMEM),
        ],
        out_specs=pl.BlockSpec(memory_space=pltpu.VMEM),
        scratch_shapes=[
            vmem((own, ao), bf16),
            vmem((own, own), bf16),
            vmem((occ_local, aux_local, ao), bf16),
            vmem((part, naux, ao), bf16),
            vmem((2, part // 2, aux_local, ao), bf16),
            vmem((naux, naux), bf16),
            vmem((depth, ao), bf16),
            vmem((ao // 4, depth), bf16),
            vmem((8, 2 * rows, depth), bf16),
            vmem((n, 8, rows, cols), F32),
            *coded(n, 6),
            *coded(n, 2),
            *coded(n, 2, 2),
            vmem((n, 2, rows, cols), F32),
            *coded(n, 2),
            *coded(n, 2, height=rows // 2),
            *coded(n, 2),
            *coded(n, 2, 2),
            *coded(n),
            *coded(8),
            vmem((rows, cols), F32),
            *coded(2, height=2 * rows, width=2 * cols // 3),
            *coded(2, height=2 * rows, width=2 * cols // 3),
        ]
        + [dma((8,))] * 3
        + [dma((4, 2))] * 3
        + [dma((16,)), dma((n, 2, 2)), dma((n, 2, 2, 2))]
        + [dma((n, 2, 2, 2)), dma((n, 2, 2))]
        + [dma((n, 2, 2)), dma((n, 2, 2, 2))]
        + [dma((n, 2)), dma((8, 2)), dma((2, 2)), dma((2, 2))],
        compiler_params=pltpu.CompilerParams(
            collective_id=0, has_side_effects=True, vmem_limit_bytes=66 * 1000 * 1000
        ),
    )(half.reshape(own, ao), metric, survive.reshape(1, -1))


def solution(mesh):
    full = mesh.shape["aux"] == 8 and mesh.shape["orb"] == 16
    return jax.shard_map(
        cube if full else plain,
        mesh=mesh,
        in_specs=(P("aux", "orb", None), P("aux", None), P("aux", "orb", None)),
        out_specs=P("orb", "aux"),
        check_vma=False,
    )
```

```python
import functools

import jax
import jax.numpy as jnp
from jax import lax
from jax.experimental import pallas as pl
from jax.experimental.pallas import tpu as pltpu
from jax.sharding import PartitionSpec as P

MESH = pl.DeviceIdType.MESH
F32 = jnp.float32


def gated(half, survive):
    aux_local, occ_local, ao_count = half.shape
    blocks_aux, blocks_occ, blocks_ao = survive.shape
    gate = survive.astype(jnp.bfloat16)
    shaped = half.reshape(
        blocks_aux, aux_local, blocks_occ, occ_local // blocks_occ, blocks_ao, ao_count // blocks_ao
    )
    return (shaped * gate[:, None, :, None, :, None]).reshape(aux_local, occ_local, ao_count)


def plain(half, metric, survive):
    aux_local, occ_local, ao_count = half.shape
    portion = lax.all_gather(gated(half, survive), "aux", axis=0, tiled=True)
    fit_total = jnp.dot(metric, portion.reshape(portion.shape[0], -1), preferred_element_type=F32)
    fitted = fit_total.astype(jnp.bfloat16).reshape(aux_local, occ_local, ao_count)
    group_width = ao_count // lax.axis_size("orb")
    row_start = lax.axis_index("orb") * group_width
    flat_rows = lax.all_gather(fitted, "orb", axis=1, tiled=True).reshape(-1, ao_count)
    left_rows = lax.dynamic_slice_in_dim(flat_rows, row_start, group_width, 1)
    partial_k = lax.dot_general(
        left_rows, flat_rows, (((0,), (0,)), ((), ())), preferred_element_type=F32
    )
    return lax.psum_scatter(partial_k, "aux", scatter_dimension=1, tiled=True)


WAVES = (
    (0, (0, 0), 0), (0, (1, 1), 0), (0, (0, 2), 1), (1, (3, 3), 0), (0, (2, 0), 1),
    (1, (1, 1), 0), (2, (2, 2), 2), (1, (3, 3), 1), (1, (0, 0), 1),
)
PLAN = (
    "r0", "n0", "r1", "n1", "g0", "r2", "q0", "n2", "g1", "r3", "q1", "a0", "n3", "a1",
    "g2", "g3", "q2", "a2", "b0", "b1", "q3", "a3", "a4", "a5", "b2", "c0", "a6", "b3",
    "c1", "a7", "b4", "c2", "d0", "a8", "b5", "c3", "d1", "b6", "c4", "d2", "e0", "b7",
    "c5", "d3", "e1", "b8", "c6", "d4", "e2", "f0", "c7", "d5", "e3", "f1", "c8", "d6",
    "e4", "f2", "d7", "e5", "f3", "d8", "e6", "f4", "e7", "f5", "e8", "f6", "f7", "f8",
)
CODES = 32767.0


def side(kind, half_of_x):
    return half_of_x if kind == 2 else kind


def block_at(x, side_of):
    return 2 * x + (x + side_of) % 2


def encode(tile, codes, scale):
    size = jnp.abs(tile)
    lanes = scale.shape[1]
    parts = tile.shape[1] // lanes
    peak = functools.reduce(jnp.maximum, [size[:, n * lanes : (n + 1) * lanes] for n in range(parts)])
    peak = jnp.maximum(jnp.max(peak, axis=0, keepdims=True), 1e-30)
    scale[...] = peak * (1.0 / CODES)
    grow = jnp.concatenate([CODES / peak] * parts, axis=1)
    codes[...] = jnp.round(tile * grow).astype(jnp.int32).astype(codes.dtype)


def decode(codes, scale):
    parts = codes.shape[1] // scale.shape[1]
    grow = jnp.concatenate([scale[...]] * parts, axis=1)
    return codes[...].astype(jnp.int32).astype(F32) * grow


def cube_kernel(
    half_ref, metric_ref, survive_ref, out_ref, raw, pick, blocks, held, via, whole, fit, turned, left,
    kf, q1, c1, far1, cf1, p1, cp1, v, q3, c3, far2, cf2, q4, c4, p2, cp2, ks, cks, fin, cfin, kept, acc, cacc, mirror,
    cmirror,
    ins, bulk, mr, zfr, znr, zrr, dr, f1r, p1r, f2s, f2r, p2s, p2r, zs, zr, xs, xr,
):
    a, o = lax.axis_index("aux"), lax.axis_index("orb")
    z, c = a // 2, a % 2
    x, y = o // 4, o % 4
    ao = fit.shape[1]
    n_own, part = blocks.shape[1], blocks.shape[0] // 4
    cut = part // 2
    naux = whole.shape[0]
    chunk, cols, rows = ao // 4, ao // 8, ao // 32
    split = rows // 2
    f_step, s_step = 4 - 3 * c, 1 + 3 * c
    f = x * (1 - c) + y * c
    s = y * (1 - c) + x * c
    partner = a + 1 - 2 * c

    def at_block(p):
        return pl.ds(p * cols, cols) if isinstance(p, int) else pl.ds(pl.multiple_of(p * cols, cols), cols)

    loads = []
    for p in range(8):
        load = pltpu.make_async_copy(
            half_ref.at[:, at_block(block_at(p % 4, p // 4))], raw.at[:, at_block(p)], ins.at[p]
        )
        load.start()
        loads.append(load)

    def orb_at(df, dsec):
        return ((f + df) % 4) * f_step + ((s + dsec) % 4) * s_step

    def aux_at(dz):
        return ((z + dz) % 4) * 2 + c

    mirrored = o // 2 != a
    peers = [(2 * a + h, o // 2) for h in range(2)]
    barrier = pltpu.get_barrier_semaphore()

    def greet(there_a, there_o):
        pl.semaphore_signal(barrier, inc=1, device_id={"aux": there_a, "orb": there_o}, device_id_type=MESH)

    for d in range(1, 8):
        greet((a + d) % 8, o)
    for d in (1, 3):
        greet(a, orb_at(d, 0))
        greet(a, orb_at(0, d))

    def remote(src, dst, send, recv, to_a, to_o):
        return pltpu.make_async_remote_copy(
            src_ref=src, dst_ref=dst, send_sem=send, recv_sem=recv,
            device_id={"aux": to_a, "orb": to_o}, device_id_type=MESH,
        )

    def go(copy):
        copy.start()
        return copy

    depth = raw.shape[0]
    orbs = blocks.shape[0]
    row_of = lax.broadcasted_iota(jnp.int32, (depth, depth), 0)
    col_of = lax.broadcasted_iota(jnp.int32, (depth, depth), 1)
    shift = n_own.bit_length() - 1
    wanted = jnp.bitwise_and(row_of, n_own - 1) * orbs + jnp.right_shift(row_of, shift)
    pick[...] = jnp.where(wanted == col_of, 1.0, 0.0).astype(pick.dtype)

    def prepare(k):
        for p in (2 * k, 2 * k + 1):
            loads[p].wait()
            block = block_at(p % 4, p // 4)
            ordered = jnp.dot(pick[...], raw[:, at_block(p)], preferred_element_type=F32)
            for n in range(cols // 128):
                gate = survive_ref[0, block * (cols // 128) + n].astype(F32)
                kept = ordered[:, n * 128 : (n + 1) * 128] * gate
                blocks[:, :, pl.ds(p * cols + n * 128, 128)] = kept.astype(blocks.dtype).reshape(orbs, n_own, 128)

    def aux_rows(aux):
        return pl.ds(pl.multiple_of(aux * n_own, n_own), n_own)

    mine = aux_rows(a)
    span = [pl.ds(k * chunk, chunk) for k in range(4)]

    def orbitals(dz, first, count):
        return pl.ds(((z + dz) % 4) * part + first, count)

    far, near, relay, to_partner = {}, {}, {}, {}

    def issue(k):
        far[k] = [
            go(remote(blocks.at[orbitals(2, 0, cut), :, span[k]], via.at[0, :, :, span[k]],
                      bulk.at[0], zfr.at[k, 0], aux_at(1), o)),
            go(remote(blocks.at[orbitals(2, cut, cut), :, span[k]], via.at[1, :, :, span[k]],
                      bulk.at[0], zfr.at[k, 1], aux_at(3), o)),
        ]
        near[k] = [
            go(remote(blocks.at[orbitals(dz, 0, part), :, span[k]], held.at[:, mine, span[k]],
                      bulk.at[0], znr.at[k, n], aux_at(dz), o))
            for n, dz in enumerate((1, 3))
        ]
        own = blocks.at[orbitals(0, 0, part), :, span[k]]
        to_partner[k, 3] = go(remote(own, held.at[:, mine, span[k]], bulk.at[0], dr.at[4 * k + 3], partner, o))
        held[:, mine, span[k]] = own[...]

    prepare(0)
    pl.semaphore_wait(barrier, 11)
    issue(0)
    prepare(1)
    issue(1)
    gather = [
        go(remote(metric_ref, whole.at[mine], bulk.at[3], mr.at[d], (a + d) % 8, o)) for d in range(1, 8)
    ]
    whole[mine, :] = metric_ref[...]
    prepare(2)
    prepare(3)

    def hand_over(k, n, dz):
        there = held.at[:, aux_rows(aux_at(dz)), span[k]]
        to_partner[k, n] = go(remote(there, there, bulk.at[2], dr.at[4 * k + n], partner, o))

    def gathered(k):
        for copy in relay[k]:
            copy.wait_recv()
        hand_over(k, 2, 2)

    def finish(k):
        if k == 0:
            for copy in gather:
                copy.wait_recv()
        for n in range(4):
            to_partner[k, n].wait_recv()

        for i in range(part):
            fit[i * naux : (i + 1) * naux, span[k]] = jnp.dot(
                whole[...], held[i, :, span[k]], preferred_element_type=F32
            ).astype(fit.dtype)
        for t in range(chunk // 128):
            turned[t * 128 : (t + 1) * 128, :] = fit[:, k * chunk + t * 128 : k * chunk + (t + 1) * 128].T

        for n in range(4):
            at = pl.ds(pl.multiple_of((2 * n + c) * rows, rows), rows)
            left[2 * k + n // 2, (n % 2) * rows : (n % 2 + 1) * rows, :] = turned[at, :]

    def pass_on(k):
        for copy in far[k]:
            copy.wait_recv()
        relay[k] = [
            go(remote(via.at[0, :, :, span[k]], held.at[pl.ds(0, cut), aux_rows(aux_at(3)), span[k]],
                      bulk.at[1], zrr.at[k, 0], aux_at(1), o)),
            go(remote(via.at[1, :, :, span[k]], held.at[pl.ds(cut, cut), aux_rows(aux_at(1)), span[k]],
                      bulk.at[1], zrr.at[k, 1], aux_at(3), o)),
        ]
        if k + 2 < 4:
            issue(k + 2)

    def take(k):
        for copy in near[k]:
            copy.wait_recv()
        hand_over(k, 0, 3)
        hand_over(k, 1, 1)

    def target(w, dest, u):
        kind = WAVES[w][0]
        by_x = 2 * ((dest % 2 + side(kind, dest // 2)) % 2) + u
        by_y = 2 * u + (dest // 2 + side(kind, u)) % 2
        return by_x * (1 - c) + by_y * c

    def tile_of(w, df, u):
        dest = (f + df) % 4
        return (2 * dest + u) * (1 - c) + (2 * target(w, dest, u) + dest % 2) * c

    def turn(w, u):
        return (target(w, f, u) + 4 - s) % 4

    def multiply(w):
        rk, step, ck = WAVES[w]

        @pl.loop(0, 4, unroll=True)
        def _(g):
            p = 4 * side(rk, g // 2) + g
            q = 4 * side(ck, g // 2) + (g + step[0] + (step[1] - step[0]) * (g // 2)) % 4
            more = jnp.dot(left[p], fit[:, at_block(q)], preferred_element_type=F32)
            kf[w, 2 * g] = more[:rows]
            kf[w, 2 * g + 1] = more[rows:]

    def both(src, src_scale, dst, dst_scale, send, recv, to_o):
        return [
            remote(src, dst, send[0], recv.at[0], a, to_o),
            remote(src_scale, dst_scale, send[1], recv.at[1], a, to_o),
        ]

    first_far, first_in, second_far, second_in, to_owner = {}, {}, {}, {}, {}

    def ring_send(w, n, u, up):
        d = 0 if up else 1
        first_in[w, u, d] = [go(copy) for copy in both(
            q1.at[w, n], c1.at[w, n], p1.at[w, u, d], cp1.at[w, u, d], (bulk.at[4], bulk.at[5]), p1r.at[w, u, d],
            orb_at(1 if up else 3, 0),
        )]

    def stage1(w):
        multiply(w)
        for u, up in ((0, True), (1, False)):
            encode(kf[w, tile_of(w, 2, u)], q1.at[w, u], c1.at[w, u])
            first_far[w, u] = [go(copy) for copy in both(
                q1.at[w, u], c1.at[w, u], far1.at[w, u], cf1.at[w, u], (bulk.at[4], bulk.at[5]), f1r.at[w, u],
                orb_at(1 if up else 3, 0),
            )]
        for u, up in ((1, True), (0, False)):
            encode(kf[w, tile_of(w, 1 if up else 3, u)], q1.at[w, 2 + u], c1.at[w, 2 + u])
            ring_send(w, 2 + u, u, up)

    def stage2(w):
        for u, up in ((0, True), (1, False)):
            for copy in first_far[w, u]:
                copy.wait_recv()
            encode(
                kf[w, tile_of(w, 1 if up else 3, u)] + decode(far1.at[w, u], cf1.at[w, u]),
                q1.at[w, 4 + u], c1.at[w, 4 + u],
            )
            ring_send(w, 4 + u, u, up)

    def stage3(w):
        for u in range(2):
            total = kf[w, tile_of(w, 0, u)]
            for d in range(2):
                for copy in first_in[w, u, d]:
                    copy.wait_recv()
                total = total + decode(p1.at[w, u, d], cp1.at[w, u, d])
            v[w, u] = total
            second_far[w, u] = [
                both(
                    q3.at[w, u, pl.ds(d * split, split)], c3.at[w, u], far2.at[w, u], cf2.at[w, u],
                    (f2s.at[w, u, 0, d], f2s.at[w, u, 1, d]), f2r.at[w, u], orb_at(0, 1 + 2 * d),
                )
                for d in range(2)
            ]

            @pl.when(turn(w, u) == 2)
            def _():
                encode(total, q3.at[w, u], c3.at[w, u])
                for pair in second_far[w, u]:
                    for copy in pair:
                        copy.start()

    def stage4(w):
        for u in range(2):
            r = turn(w, u)
            late = jnp.where(r == 3, 1, 0)
            second_in[w, u] = both(
                q4.at[w, u], c4.at[w, u], p2.at[w, u, late], cp2.at[w, u, late],
                (p2s.at[w, u, 0], p2s.at[w, u, 1]), p2r.at[w, u, late], orb_at(0, r),
            )

            @pl.when(r % 2 == 1)
            def _():
                for copy in second_far[w, u][0]:
                    copy.wait_recv()
                at = pl.ds(pl.multiple_of(late * split, split), split)
                v[w, u, at] += decode(far2.at[w, u], cf2.at[w, u])
                encode(v[w, u], q4.at[w, u], c4.at[w, u])
                for copy in second_in[w, u]:
                    copy.start()

    def owner_of(w):
        step, ck = WAVES[w][1:]
        there = (x + step[0] + (step[1] - step[0]) * (x // 2)) % 4
        return 2 * there + (there + side(ck, x // 2)) % 2

    own_side = (x + y // 2) % 2

    def owned(w):
        return jnp.logical_and(own_side == side(WAVES[w][0], x // 2), owner_of(w) == a)

    def stage5(w):
        owner = owner_of(w)
        d = (owner + 8 - a) % 8
        to_owner[w] = [
            remote(ks.at[w], fin.at[d], zs.at[w, 0], zr.at[d, 0], owner, o),
            remote(cks.at[w], cfin.at[d], zs.at[w, 1], zr.at[d, 1], owner, o),
        ]
        for u in range(2):

            @pl.when(turn(w, u) == 0)
            def _():
                total = v[w, u]
                for n in range(2):
                    for copy in both(
                        q4.at[w, u], c4.at[w, u], p2.at[w, u, n], cp2.at[w, u, n], (p2s.at[w, u, 0], p2s.at[w, u, 1]), p2r.at[w, u, n], o
                    ):
                        copy.wait_recv()
                    total = total + decode(p2.at[w, u, n], cp2.at[w, u, n])

                @pl.when(owner != a)
                def _():
                    encode(total, ks.at[w], cks.at[w])
                    for copy in to_owner[w]:
                        copy.start()

                @pl.when(owner == a)
                def _():
                    kept[...] = total

    half_cols = 2 * cols // 3

    def place(c_rows):
        return pl.ds(pl.multiple_of(c_rows * rows, rows), rows)

    outgoing = [
        [
            remote(acc.at[h], mirror.at[o % 2], xs.at[h, 0], xr.at[o % 2, 0], peers[h][1], peers[h][0]),
            remote(cacc.at[h], cmirror.at[o % 2], xs.at[h, 1], xr.at[o % 2, 1], peers[h][1], peers[h][0]),
        ]
        for h in range(2)
    ]

    def stage6(w):
        for u in range(2):
            r = turn(w, u)

            @pl.when(r == 2)
            def _():
                for pair in second_far[w, u]:
                    for copy in pair:
                        copy.wait_send()

            @pl.when(r % 2 == 1)
            def _():
                for copy in second_in[w, u]:
                    copy.wait_send()

        @pl.when(owned(w))
        def _():
            for d in range(1, 8):
                remote(ks.at[0], fin.at[d], zs.at[0, 0], zr.at[d, 0], a, o).wait_recv()
                remote(cks.at[0], cfin.at[d], zs.at[0, 1], zr.at[d, 1], a, o).wait_recv()
            part_of = [decode(fin.at[d], cfin.at[d]) for d in range(1, 8)]
            out_ref[place(c), :] = kept[...] + part_of[1] + part_of[3] + part_of[5]
            out_ref[place(1 - c), :] = part_of[0] + part_of[2] + part_of[4] + part_of[6]
            if sum(WAVES[w][1]) or WAVES[w][0] != WAVES[w][2]:
                for h, pair in enumerate(outgoing):
                    first = h * (cols - half_cols)
                    encode(out_ref[:, first : first + half_cols], acc.at[h], cacc.at[h])
                    for copy in pair:
                        copy.start()

    count = len(WAVES)

    calls = dict(
        r=pass_on, n=take, g=gathered, q=finish, a=stage1, b=stage2, c=stage3, d=stage4, e=stage5, f=stage6
    )
    for name in PLAN:
        calls[name[0]](int(name[1]))
    direct = functools.reduce(jnp.logical_or, [owned(w) for w in range(count)])

    sent = (blocks, via, held.at[:, pl.ds(0, 3 * n_own)], whole.at[pl.ds(0, 7 * n_own)], q1, c1)
    for n, ref in enumerate(sent):
        remote(ref, ref, bulk.at[n], xr.at[0, 0], a, o).wait_send()
    for w in range(count):

        @pl.when(jnp.logical_and(jnp.logical_or(turn(w, 0) == 0, turn(w, 1) == 0), owner_of(w) != a))
        def _():
            for copy in to_owner[w]:
                copy.wait_send()

    @pl.when(jnp.logical_not(direct))
    def _():
        for h in range(2):
            remote(acc.at[h], mirror.at[h], xs.at[h, 0], xr.at[h, 0], a, o).wait_recv()
            remote(cacc.at[h], cmirror.at[h], xs.at[h, 1], xr.at[h, 1], a, o).wait_recv()
        across = jnp.concatenate([decode(mirror.at[h], cmirror.at[h]) for h in range(2)], axis=0).T

        @pl.when(o % 2 == 0)
        def _():
            out_ref[...] = across[: 2 * rows]

        @pl.when(o % 2 == 1)
        def _():
            out_ref[...] = across[half_cols - 2 * rows :]

    @pl.when(jnp.logical_and(direct, mirrored))
    def _():
        for pair in outgoing:
            for copy in pair:
                copy.wait_send()


def cube(half, metric, survive):
    aux_local, occ_local, ao = half.shape
    naux = 8 * aux_local
    part = occ_local // 4
    depth = part * naux
    own = aux_local * occ_local
    rows, cols = ao // 32, ao // 8
    n = len(WAVES)
    dma, vmem = pltpu.SemaphoreType.DMA, pltpu.VMEM
    bf16, i16 = jnp.bfloat16, jnp.int16

    def coded(*lead, height=rows, width=cols):
        return [vmem((*lead, height, width), i16), vmem((*lead, 1, 128), F32)]

    return pl.pallas_call(
        cube_kernel,
        out_shape=jax.ShapeDtypeStruct((2 * rows, cols), F32),
        in_specs=[
            pl.BlockSpec(memory_space=pl.ANY),
            pl.BlockSpec(memory_space=pltpu.VMEM),
            pl.BlockSpec(memory_space=pltpu.SMEM),
        ],
        out_specs=pl.BlockSpec(memory_space=pltpu.VMEM),
        scratch_shapes=[
            vmem((own, ao), bf16),
            vmem((own, own), bf16),
            vmem((occ_local, aux_local, ao), bf16),
            vmem((part, naux, ao), bf16),
            vmem((2, part // 2, aux_local, ao), bf16),
            vmem((naux, naux), bf16),
            vmem((depth, ao), bf16),
            vmem((ao // 4, depth), bf16),
            vmem((8, 2 * rows, depth), bf16),
            vmem((n, 8, rows, cols), F32),
            *coded(n, 6),
            *coded(n, 2),
            *coded(n, 2, 2),
            vmem((n, 2, rows, cols), F32),
            *coded(n, 2),
            *coded(n, 2, height=rows // 2),
            *coded(n, 2),
            *coded(n, 2, 2),
            *coded(n),
            *coded(8),
            vmem((rows, cols), F32),
            *coded(2, height=2 * rows, width=2 * cols // 3),
            *coded(2, height=2 * rows, width=2 * cols // 3),
        ]
        + [dma((8,))] * 3
        + [dma((4, 2))] * 3
        + [dma((16,)), dma((n, 2, 2)), dma((n, 2, 2, 2))]
        + [dma((n, 2, 2, 2)), dma((n, 2, 2))]
        + [dma((n, 2, 2)), dma((n, 2, 2, 2))]
        + [dma((n, 2)), dma((8, 2)), dma((2, 2)), dma((2, 2))],
        compiler_params=pltpu.CompilerParams(
            collective_id=0, has_side_effects=True, vmem_limit_bytes=66 * 1000 * 1000
        ),
    )(half.reshape(own, ao), metric, survive.reshape(1, -1))


def solution(mesh):
    full = mesh.shape["aux"] == 8 and mesh.shape["orb"] == 16
    return jax.shard_map(
        cube if full else plain,
        mesh=mesh,
        in_specs=(P("aux", "orb", None), P("aux", None), P("aux", "orb", None)),
        out_specs=P("orb", "aux"),
        check_vma=False,
    )
```
